32 devices in a mesh: row: 4 (over y, x), col: 8 (over z, core).
Axes of the slice: x: 2, y: 2, z: 4, core: 2. Of those that a mesh axis runs over, the one named last changes fastest.
Arguments:
- object_field: float32 [2, 1024, 2048], P(None, 'row', 'col'), may hold values from -6 to 6
- probe_modes: float32 [4, 2, 256, 256], replicated, may hold values from -3 to 3
- positions: int32 [4, 8, 6, 2], P('row', 'col'), may hold values from 0 to 255
- counts: int32 [4, 8], P('row', 'col'), may hold values from 0 to 6, as said below
- amplitude: float32 [4, 8, 6, 256, 256], P('row', 'col'), may hold values from 0 to 2
Outputs:
- updated: float32 [2, 1024, 2048], P(None, 'row', 'col')
The draws below stay inside these ranges and needn't reach their ends.
Inputs may be any that keep to these rules, and one draw needn't show every extreme that they name: The counts of two tiles in one tile row whose column indices differ by 4 add up to 6; some tile has exactly 6. Only positions below a tile's count are used.
All inputs are finite; a program needn't handle non-finite values.
Results may differ from the reference program's by a relative error of at most 0.0018.
Values sent between devices are 32-bit elements; how exact they have to be, the bound alone decides.
A program may use at most 64 MiB of HBM per device.

```python
import math
import jax
import jax.numpy as jnp
from jax import lax

PATCH = 256
MODES = 4
TILE = 256
SLOTS = 3
ITERS = 2
SURPLUS = 3
MOST = 6
TILES_R = 4
TILES_C = 8
ROWS = 1024
COLS = 2048


def draw_counts(key, part):
    half = TILES_C // 2
    first = jax.random.fold_in(key, 11)
    second = jax.random.fold_in(key, 23)
    base = jax.random.randint(first, (TILES_R, half), SLOTS - SURPLUS, SLOTS + SURPLUS + 1)
    spot = jax.random.randint(second, (), 0, TILES_R * half)
    flat = jnp.where(jnp.arange(TILES_R * half) == spot, MOST, base.reshape(-1))
    base = flat.reshape(TILES_R, half)
    return jnp.concatenate([base, 2 * SLOTS - base], axis=1).astype(jnp.int32)


def set_ends(result, own_key, least, top_value):
    longest = result.shape.index(max(result.shape))
    spots = []
    for shift in (0, 1):
        where = [jax.random.randint(jax.random.fold_in(own_key, axis), (), 0, length) for axis, length in enumerate(result.shape)]
        where[longest] = (where[longest] + shift) % result.shape[longest]
        spots.append(tuple(where))
    return result.at[spots[0]].set(least).at[spots[1]].set(top_value)


def shard_levels(key, dims, split, least, largest):
    def one(dim, shards_of):
        heights = jax.random.uniform(jax.random.fold_in(jax.random.fold_in(key, 6), dim), (shards_of,), jnp.float32, least / len(split), largest / len(split))
        return jnp.repeat(jnp.exp(heights), dims[dim] // shards_of).reshape((-1,) + (1,) * (len(dims) - dim - 1))

    gain = one(*split[0])
    for cut in split[1:]:
        gain = gain * one(*cut)
    return gain


def scatter_about(key, extent, deviation, most, shards=(), held_as=jnp.bfloat16):
    entries = jax.random.normal(key, extent, jnp.float32) * deviation
    if len(shards) > 0:
        entries = shard_levels(key, extent, shards, -0.22, 0.18) * entries
    return jnp.clip(entries, min=-most, max=most).astype(held_as)


def setup_inputs(seed: int = 0) -> dict:
    splits = jax.random.split(jax.random.key(seed), 6)
    return {
        "object_field": scatter_about(splits[0], (2, ROWS, COLS), 1.0, 6.0, ((1, 4), (2, 8)), jnp.float32),
        "probe_modes": scatter_about(splits[1], (MODES, 2, PATCH, PATCH), 0.5, 3.0, (), jnp.float32),
        "positions": set_ends(jax.random.randint(splits[2], (TILES_R, TILES_C, MOST, 2), 0, TILE), jax.random.fold_in(splits[2], 1), 0, TILE - 1).astype(jnp.int32),
        "counts": draw_counts(jax.random.fold_in(splits[5], 71), 0),
        "amplitude": jnp.clip(2.0 * jax.random.uniform(splits[4], (TILES_R, TILES_C, MOST, PATCH, PATCH), jnp.float32) ** shard_levels(splits[4], (TILES_R, TILES_C, MOST, PATCH, PATCH), ((0, 4), (1, 8)), -0.2, 0.2), 0.0, 2.0),
    }


step_size = 0.1
damping = 0.1

def blocks(upper_left, upper_right, lower_left, lower_right):
    return jnp.stack([jnp.stack([upper_left, upper_right], axis=1), jnp.stack([lower_left, lower_right], axis=1)], axis=0)

def tables():
    ladder = jnp.arange(PATCH, dtype=jnp.int32)
    product = ladder[:, None] * ladder[None, :] % PATCH
    theta = product.astype(jnp.float32) * (2.0 * math.pi / PATCH)
    factor = 1.0 / math.sqrt(PATCH)
    cosine = jnp.cos(theta) * factor
    minus_sine = -jnp.sin(theta) * factor
    table_fwd = blocks(cosine, -minus_sine, minus_sine, cosine).astype(jnp.bfloat16)
    table_inv = blocks(cosine, minus_sine, -minus_sine, cosine).astype(jnp.bfloat16)
    return (table_fwd, table_inv)

def left_mult(table, values):
    return jnp.einsum('cjdk,mdkl->mcjl', table.astype(jnp.float32), values.astype(jnp.float32), precision=lax.Precision.HIGHEST)

def right_mult(values, table):
    return jnp.einsum('mcjk,ckdl->mdjl', values.astype(jnp.float32), table.astype(jnp.float32), precision=lax.Precision.HIGHEST)

def patch_gradient(patch, measured, probe_modes, table_fwd, table_inv):
    probe_re = probe_modes[:, 0]
    probe_im = probe_modes[:, 1]
    psi = jnp.stack([probe_re * patch[0] - probe_im * patch[1], probe_re * patch[1] + probe_im * patch[0]], axis=1).astype(jnp.bfloat16)
    section = left_mult(table_fwd, psi).astype(jnp.bfloat16)
    far = right_mult(section, table_inv)
    intensity = lax.optimization_barrier(jnp.sum(far * far, axis=(0, 1)))
    ratio = 1.0 - measured / jnp.sqrt(intensity + damping)
    chi = (far * ratio).astype(jnp.bfloat16)
    back = left_mult(table_inv, chi).astype(jnp.bfloat16)
    wave = right_mult(back, table_fwd)
    grad_re = lax.optimization_barrier(jnp.sum(probe_re * wave[:, 0] + probe_im * wave[:, 1], axis=0))
    grad_im = lax.optimization_barrier(jnp.sum(probe_re * wave[:, 1] - probe_im * wave[:, 0], axis=0))
    return jnp.stack([grad_re, grad_im], axis=0)

def reference(object_field, probe_modes, positions, counts, amplitude):
    table_fwd, table_inv = tables()
    tile_rows, tile_cols = counts.shape
    slot_ids = jnp.arange(MOST, dtype=jnp.int32)
    live = (slot_ids[None, None, :] < counts[:, :, None]).reshape(-1)
    order = jnp.argsort(jnp.where(live, 0, 1).astype(jnp.int32), stable=True)[:SLOTS * tile_rows * tile_cols].astype(jnp.int32)
    tile_row = order // (tile_cols * MOST)
    tile_col = order // MOST % tile_cols
    offsets = positions.reshape(-1, 2)
    top_rows = (tile_row * TILE + offsets[order, 0]).astype(jnp.int32)
    left_cols = (tile_col * TILE + offsets[order, 1]).astype(jnp.int32)
    measured_all = amplitude.reshape(-1, PATCH, PATCH)
    anchor = jnp.int32(0)
    field = object_field
    for sweep in range(ITERS):
        padded = jnp.pad(field, ((0, 0), (0, PATCH), (0, PATCH)))

        def visit(total, entry):
            which, top, left = entry
            patch = lax.dynamic_slice(padded, (anchor, top, left), (2, PATCH, PATCH))
            measured = lax.dynamic_index_in_dim(measured_all, which, 0, keepdims=False)
            grads = patch_gradient(patch, measured, probe_modes, table_fwd, table_inv)
            current = lax.dynamic_slice(total, (anchor, top, left), (2, PATCH, PATCH))
            return (lax.dynamic_update_slice(total, current + grads, (anchor, top, left)), None)
        total, unused = lax.scan(visit, jnp.zeros_like(padded), (order, top_rows, left_cols))
        field = field - step_size * total[:, :ROWS, :COLS]
    return field
```

```python
import functools
import math

import jax
import jax.numpy as jnp
import numpy as np
from jax import lax
from jax.experimental import pallas as pl
from jax.experimental.pallas import tpu as pltpu
from jax.sharding import PartitionSpec as P

ITERS = 2


step_size = 0.1
damping = 0.1


RIGHT_LOW, RIGHT_TOP, DOWN, UP, LEFT, LEFT_LOW = range(6)
PARTS = 4


def exchange_kernel(mode, rows_of, cols_of, *refs):
    refs = list(refs)
    reduce, spread = mode != "spread", mode != "reduce"
    if reduce:
        tot_ref, ext_ref, out_ref = refs.pop(0), refs.pop(0), refs.pop(0)
        side_scr, top_scr, low_scr, above_scr = [refs.pop(0) for _ in range(4)]
        below_scr = refs.pop(0) if spread else None
        t = out_ref.shape[-1]
    else:
        field_ref, amp_ref = refs.pop(0), refs.pop(0)
        out_ref, sorted_ref, amp_scr, perm_scr, local_sem = [refs.pop(0) for _ in range(5)]
        t = field_ref.shape[-1]
    send_sem, recv_sem = refs
    chunk = t // PARTS
    r, c = lax.axis_index("row"), lax.axis_index("col")
    has_up, has_down = r > 0, r < rows_of - 1
    has_left, has_right = c > 0, c < cols_of - 1
    up = (jnp.where(has_up, r - 1, r + 1), c)
    down = (jnp.where(has_down, r + 1, r - 1), c)
    left = (r, jnp.where(has_left, c - 1, c + 1))
    right = (r, jnp.where(has_right, c + 1, c - 1))

    if not reduce:
        own = pltpu.make_async_copy(field_ref, out_ref.at[0, :, pl.ds(0, t)], local_sem.at[0])
        own.start()
        measured = pltpu.make_async_copy(amp_ref, amp_scr, local_sem.at[1])
        measured.start()

    barrier = pltpu.get_barrier_semaphore()
    for there, device in ((has_up, up), (has_down, down), (has_left, left), (has_right, right)):

        @pl.when(there)
        def _():
            pl.semaphore_signal(
                barrier, inc=1, device_id=device, device_id_type=pl.DeviceIdType.MESH
            )

    peers = sum(jnp.where(there, 1, 0) for there in (has_up, has_down, has_left, has_right))
    pl.semaphore_wait(barrier, peers)

    def copy(kind, i):
        rows = pl.ds(i * chunk, chunk)
        low = pl.ds(t + i * chunk, chunk)
        if kind == RIGHT_LOW:
            src, dst, device = tot_ref.at[1, :, low], side_scr.at[:, low], right
        elif kind == RIGHT_TOP:
            src, dst, device = tot_ref.at[1, :, rows], side_scr.at[:, rows], right
        elif kind == DOWN:
            src, dst, device = low_scr.at[:, rows], above_scr.at[:, rows], down
        elif kind == UP and reduce:
            src, dst, device = top_scr.at[:, rows], below_scr.at[:, rows], up
        elif kind == UP:
            src, dst, device = field_ref.at[:, rows], out_ref.at[0, :, low], up
        elif kind == LEFT and reduce:
            src, dst, device = out_ref.at[0, :, rows], out_ref.at[1, :, rows], left
        elif kind == LEFT:
            src, dst, device = field_ref.at[:, rows], out_ref.at[1, :, rows], left
        else:
            src, dst, device = out_ref.at[0, :, low], out_ref.at[1, :, low], left
        return pltpu.make_async_remote_copy(
            src_ref=src,
            dst_ref=dst,
            send_sem=send_sem.at[kind, i],
            recv_sem=recv_sem.at[kind, i],
            device_id=device,
            device_id_type=pl.DeviceIdType.MESH,
        )

    def start(there, kind, i):
        @pl.when(there)
        def _():
            copy(kind, i).start()

    def got(there, kind, i):
        @pl.when(there)
        def _():
            copy(kind, i).wait_recv()

    def sent(there, kind):
        @pl.when(there)
        def _():
            for i in range(PARTS):
                copy(kind, i).wait_send()

    if reduce:
        for i in range(PARTS):
            start(has_right, RIGHT_LOW, i)
            if spread:
                start(has_right, RIGHT_TOP, i)
        if not spread:
            for i in range(PARTS):
                start(has_right, RIGHT_TOP, i)

        @pl.when(jnp.logical_not(has_left))
        def _():
            side_scr[...] = jnp.zeros_like(side_scr)

        @pl.when(jnp.logical_not(has_up))
        def _():
            above_scr[...] = jnp.zeros_like(above_scr)

    if spread:

        @pl.when(jnp.logical_not(has_down))
        def _():
            out_ref[0, :, t:] = jnp.zeros((2, t, t), jnp.float32)

        @pl.when(jnp.logical_not(has_right))
        def _():
            out_ref[1] = jnp.zeros((2, 2 * t, t), jnp.float32)

        @pl.when(jnp.logical_and(has_right, jnp.logical_not(has_down)))
        def _():
            out_ref[1, :, t:] = jnp.zeros((2, t, t), jnp.float32)

    def band(i):
        return slice(i * chunk, (i + 1) * chunk), slice(t + i * chunk, t + (i + 1) * chunk)

    both = jnp.logical_and(has_down, has_left)
    if reduce:
        for i in range(PARTS):
            rows, low = band(i)
            got(has_left, RIGHT_LOW, i)

            @pl.when(has_down)
            def _():
                low_scr[:, rows] = tot_ref[0, :, low] + side_scr[:, low]
                copy(DOWN, i).start()

            if spread:
                got(has_left, RIGHT_TOP, i)
                top_scr[:, rows] = tot_ref[0, :, rows] + side_scr[:, rows]
                start(has_up, UP, i)
        for i in range(PARTS):
            rows, low = band(i)
            if spread:
                got(has_up, DOWN, i)
                out_ref[0, :, rows] = ext_ref[0, :, rows] - step_size * (
                    top_scr[:, rows] + above_scr[:, rows]
                )
                start(has_left, LEFT, i)

                @pl.when(has_down)
                def _():
                    copy(UP, i).wait_recv()
                    out_ref[0, :, low] = ext_ref[0, :, low] - step_size * (
                        low_scr[:, rows] + below_scr[:, rows]
                    )

                start(both, LEFT_LOW, i)
            else:
                got(has_left, RIGHT_TOP, i)
                got(has_up, DOWN, i)
                out_ref[:, rows] = ext_ref[0, :, rows] - step_size * (
                    (tot_ref[0, :, rows] + side_scr[:, rows]) + above_scr[:, rows]
                )
    else:
        for i in range(PARTS):
            start(has_up, UP, i)
            start(has_left, LEFT, i)
        spot = lax.broadcasted_iota(jnp.int32, (t, t), 1)
        spot = jnp.where(spot < t // 2, 2 * spot, 2 * spot - (t - 1))
        perm = jnp.where(lax.broadcasted_iota(jnp.int32, (t, t), 0) == spot, 1.0, 0.0)
        perm_scr[0] = perm.astype(jnp.bfloat16)
        spot = lax.broadcasted_iota(jnp.int32, (t, t), 0)
        spot = jnp.where(spot < t // 2, 2 * spot, 2 * spot - (t - 1))
        perm = jnp.where(lax.broadcasted_iota(jnp.int32, (t, t), 1) == spot, 1.0, 0.0)
        perm_scr[1] = perm.astype(jnp.bfloat16)
        measured.wait()
        slots = amp_ref.shape[0]
        done = 0
        for i in range(PARTS):
            until = min(slots, -(-slots * (i + 1) // PARTS))

            def one(s, carry):
                cols = exact(amp_scr[s], lambda piece: dot(piece, perm_scr[0]))
                sorted_ref[s] = exact(cols, lambda piece: dot(perm_scr[1], piece))
                return carry

            lax.fori_loop(done, until, one, 0)
            done = until
            got(has_down, UP, i)
            start(both, LEFT_LOW, i)
    if not reduce:
        own.wait()
    if spread:
        for i in range(PARTS):
            got(has_right, LEFT, i)
            got(jnp.logical_and(has_right, has_down), LEFT_LOW, i)
    if reduce:
        sent(has_right, RIGHT_LOW)
        sent(has_right, RIGHT_TOP)
        sent(has_down, DOWN)
    if spread:
        sent(has_up, UP)
        sent(has_left, LEFT)
        sent(both, LEFT_LOW)


def exchange(mode, *operands):
    planes, t = operands[0].shape[-3], operands[0].shape[-1]
    vmem = pl.BlockSpec(memory_space=pltpu.VMEM)
    tile = jax.ShapeDtypeStruct((planes, t, t), jnp.float32)
    shapes = [tile if mode == "reduce" else jax.ShapeDtypeStruct((2, planes, 2 * t, t), jnp.float32)]
    specs = [vmem] * len(operands)
    if mode == "spread":
        amp = operands[1]
        specs = [pl.BlockSpec(memory_space=pltpu.HBM)] * 2
        shapes.append(jax.ShapeDtypeStruct(amp.shape, jnp.float32))
        scratch = [
            pltpu.VMEM(amp.shape, jnp.float32),
            pltpu.VMEM((2, t, t), jnp.bfloat16),
            pltpu.SemaphoreType.DMA((2,)),
        ]
    else:
        scratch = [pltpu.VMEM((planes, 2 * t, t), jnp.float32)]
        scratch += [pltpu.VMEM((planes, t, t), jnp.float32)] * (4 if mode == "both" else 3)
    scratch += [pltpu.SemaphoreType.DMA((6, PARTS))] * 2
    kernel = functools.partial(
        exchange_kernel, mode, lax.axis_size("row"), lax.axis_size("col")
    )
    return pl.pallas_call(
        kernel,
        out_shape=shapes,
        in_specs=specs,
        out_specs=[vmem] * len(shapes),
        scratch_shapes=scratch,
        compiler_params=pltpu.CompilerParams(
            collective_id=("spread", "both", "reduce").index(mode),
            has_side_effects=True,
            vmem_limit_bytes=24 * 1024 * 1024,
        ),
        name="exchange_" + mode,
    )(*operands)


def tables(width):
    half = width // 2
    ladder = np.arange(width)
    theta = (ladder[:, None] * ladder[None, :] % width) * (2.0 * math.pi / width)
    factor = 1.0 / math.sqrt(width)
    cosine = np.cos(theta) * factor
    sine = np.sin(theta) * factor
    out = []
    for parity in (0, 1):
        c = cosine[parity::2, :half]
        s = sine[parity::2, :half]
        out.append(np.block([[c, s], [-s, c]]))
    stacked = np.stack(out).astype(np.float32)
    fwd = jnp.asarray(stacked).astype(jnp.bfloat16)
    inv = jnp.asarray(np.ascontiguousarray(stacked.transpose(0, 2, 1))).astype(jnp.bfloat16)
    return fwd, inv


def dot(a, b):
    return jnp.dot(a, b, preferred_element_type=jnp.float32)


def gradient_kernel(
    count_ref,
    pos_ref,
    ext_ref,
    amp_ref,
    probe_ref,
    a_ref,
    b_ref,
    tot_ref,
    patch_scr,
    psi_scr,
    x_scr,
    far_scr,
    chi_scr,
    y_scr,
    grad_scr,
):
    modes, _, width, _ = probe_ref.shape
    h = width // 2
    lane = 128
    wide = width + lane
    tot_ref[...] = jnp.zeros_like(tot_ref)
    sub = 8
    blocks = width // sub
    step = 16

    def slot(s, carry):
        top = pos_ref[0, s]
        left = pos_ref[1, s]
        base = left // lane
        rest = left - base * lane
        over = pl.multiple_of((top // sub) * sub, sub)
        drop = top - over

        def block_of(c):
            half = (base + c) // (width // lane)
            near = base + c - half * (width // lane)
            return half, pl.ds(pl.multiple_of(near * lane, lane), lane)

        lanes = lax.broadcasted_iota(jnp.int32, (width, lane), 1)
        ledge = lax.broadcasted_iota(jnp.int32, (blocks, sub, lane), 1)
        for d in range(2):
            turned = []
            for c in range(wide // lane):
                half, cols = block_of(c)
                x = ext_ref[half, d, pl.ds(over, width + sub), cols].reshape(blocks + 1, sub, lane)
                x = pltpu.roll(x, lax.rem(sub - drop, sub), 1)
                x = jnp.where(ledge + drop < sub, x[:-1], x[1:]).reshape(width, lane)
                turned.append(pltpu.roll(x, lax.rem(lane - rest, lane), 1))
            for c in range(width // lane):
                patch_scr[d, :, c * lane : (c + 1) * lane] = jnp.where(
                    lanes + rest < lane, turned[c], turned[c + 1]
                )
        for m in range(modes):
            for r in range(0, h, step):
                rows = slice(r, r + step)
                low = slice(h + r, h + r + step)
                pr, pi = probe_ref[m, 0, rows], probe_ref[m, 1, rows]
                qr, qi = probe_ref[m, 0, low], probe_ref[m, 1, low]
                fr, fi = patch_scr[0, rows], patch_scr[1, rows]
                gr, gi = patch_scr[0, low], patch_scr[1, low]
                ur, ui = pr * fr - pi * fi, pr * fi + pi * fr
                vr, vi = qr * gr - qi * gi, qr * gi + qi * gr
                psi_scr[m, 0, rows] = (ur + vr).astype(jnp.bfloat16)
                psi_scr[m, 0, low] = (ui + vi).astype(jnp.bfloat16)
                psi_scr[m, 1, rows] = (ur - vr).astype(jnp.bfloat16)
                psi_scr[m, 1, low] = (ui - vi).astype(jnp.bfloat16)
            for p in range(2):
                out = dot(a_ref[p], psi_scr[m, p])
                re_l, re_r = out[:h, :h], out[:h, h:]
                im_l, im_r = out[h:, :h], out[h:, h:]
                rows = slice(p * h, (p + 1) * h)
                x_scr[m, 0, rows, :h] = (re_l + re_r).astype(jnp.bfloat16)
                x_scr[m, 0, rows, h:] = (im_l + im_r).astype(jnp.bfloat16)
                x_scr[m, 1, rows, :h] = (re_l - re_r).astype(jnp.bfloat16)
                x_scr[m, 1, rows, h:] = (im_l - im_r).astype(jnp.bfloat16)
            for q in range(2):
                far_scr[m, q] = dot(x_scr[m, q], b_ref[q])
        for p in range(2):
            for q in range(2):
                cols = slice(q * h, (q + 1) * h)
                for r in range(0, h, step):
                    rows = slice(p * h + r, p * h + r + step)
                    total = None
                    for m in range(modes):
                        re, im = far_scr[m, q, rows, :h], far_scr[m, q, rows, h:]
                        term = re * re + im * im
                        total = term if total is None else total + term
                    ratio = 1.0 - amp_ref[s, rows, cols] * lax.rsqrt(total + damping)
                    for m in range(modes):
                        re, im = far_scr[m, q, rows, :h], far_scr[m, q, rows, h:]
                        chi_scr[m, p, r : r + step, cols] = (re * ratio).astype(jnp.bfloat16)
                        chi_scr[m, p, h + r : h + r + step, cols] = (im * ratio).astype(
                            jnp.bfloat16
                        )
        for m in range(modes):
            even = dot(b_ref[0], chi_scr[m, 0])
            odd = dot(b_ref[1], chi_scr[m, 1])
            upper = (even + odd).astype(jnp.bfloat16)
            lower = (even - odd).astype(jnp.bfloat16)
            for q in range(2):
                cols = slice(q * h, (q + 1) * h)
                y_scr[m, q, :h, :h] = upper[:h, cols]
                y_scr[m, q, :h, h:] = upper[h:, cols]
                y_scr[m, q, h:, :h] = lower[:h, cols]
                y_scr[m, q, h:, h:] = lower[h:, cols]
            even = dot(y_scr[m, 0], a_ref[0])
            odd = dot(y_scr[m, 1], a_ref[1])
            for cols, wave in ((slice(0, h), even + odd), (slice(h, width), even - odd)):
                wr, wi = wave[:, :h], wave[:, h:]
                pr, pi = probe_ref[m, 0, :, cols], probe_ref[m, 1, :, cols]
                gr, gi = pr * wr + pi * wi, pr * wi - pi * wr
                if m > 0:
                    gr, gi = grad_scr[0, :, cols] + gr, grad_scr[1, :, cols] + gi
                grad_scr[0, :, cols] = gr
                grad_scr[1, :, cols] = gi
        for d in range(2):
            edge = jnp.zeros((width, lane), jnp.float32)
            turned = [edge]
            for c in range(width // lane):
                x = grad_scr[d, :, c * lane : (c + 1) * lane]
                turned.append(pltpu.roll(x, rest, 1))
            turned.append(edge)
            for c in range(wide // lane):
                x = jnp.where(lanes >= rest, turned[c + 1], turned[c])
                x = pltpu.roll(x.reshape(blocks, sub, lane), drop, 1)
                brim = jnp.zeros((1, sub, lane), jnp.float32)
                after = jnp.concatenate([x, brim], axis=0)
                before = jnp.concatenate([brim, x], axis=0)
                rim = lax.broadcasted_iota(jnp.int32, (blocks + 1, sub, lane), 1)
                x = jnp.where(rim >= drop, after, before).reshape(width + sub, lane)
                half, cols = block_of(c)
                spot = (half, d, pl.ds(over, width + sub), cols)
                tot_ref[spot] = tot_ref[spot] + x
        return carry

    lax.fori_loop(0, count_ref[0, 0], slot, 0)


def gradient(counts, where, extended, amp, probe_modes, fwd, inv):
    modes, _, width, _ = probe_modes.shape
    vmem = pl.BlockSpec(memory_space=pltpu.VMEM)
    smem = pl.BlockSpec(memory_space=pltpu.SMEM)
    return pl.pallas_call(
        gradient_kernel,
        out_shape=jax.ShapeDtypeStruct(extended.shape, jnp.float32),
        in_specs=[smem, smem] + [vmem] * 5,
        out_specs=vmem,
        scratch_shapes=[
            pltpu.VMEM((2, width, width), jnp.float32),
            pltpu.VMEM((modes, 2, width, width), jnp.bfloat16),
            pltpu.VMEM((modes, 2, width, width), jnp.bfloat16),
            pltpu.VMEM((modes, 2, width, width), jnp.float32),
            pltpu.VMEM((modes, 2, width, width), jnp.bfloat16),
            pltpu.VMEM((modes, 2, width, width), jnp.bfloat16),
            pltpu.VMEM((2, width, width), jnp.float32),
        ],
        compiler_params=pltpu.CompilerParams(vmem_limit_bytes=40 * 1024 * 1024),
        name="gradient",
    )(counts, where, extended, amp, probe_modes, fwd, inv)


def exact(values, product):
    total = None
    for _ in range(3):
        piece = values.astype(jnp.bfloat16)
        values = values - piece.astype(jnp.float32)
        part = product(piece)
        total = part if total is None else total + part
    return total


def body(object_field, probe_modes, positions, counts, amplitude):
    width = probe_modes.shape[-1]
    fwd, inv = tables(width)
    where = positions[0, 0].T
    held = [pltpu.with_memory_space_constraint(x, pltpu.HBM) for x in (object_field, amplitude[0, 0])]
    extended, amp = exchange("spread", *held)
    for sweep in range(ITERS):
        total = gradient(counts, where, extended, amp, probe_modes, fwd, inv)
        (extended,) = exchange("both" if sweep < ITERS - 1 else "reduce", total, extended)
    return extended


def solution(mesh):
    placed = (
        P(None, "row", "col"),
        P(),
        P("row", "col", None, None),
        P("row", "col"),
        P("row", "col", None, None, None),
    )
    return jax.shard_map(
        body, mesh=mesh, in_specs=placed, out_specs=P(None, "row", "col"), check_vma=False
    )
```

```python
import functools
import math

import jax
import jax.numpy as jnp
import numpy as np
from jax import lax
from jax.experimental import pallas as pl
from jax.experimental.pallas import tpu as pltpu
from jax.sharding import PartitionSpec as P

ITERS = 2


step_size = 0.1
damping = 0.1


RIGHT_LOW, RIGHT_TOP, DOWN, UP, LEFT, LEFT_LOW = range(6)
PARTS = 4


def exchange_kernel(mode, rows_of, cols_of, *refs):
    refs = list(refs)
    reduce, spread = mode != "spread", mode != "reduce"
    if reduce:
        tot_ref, ext_ref, out_ref = refs.pop(0), refs.pop(0), refs.pop(0)
        side_scr, top_scr, low_scr, above_scr = [refs.pop(0) for _ in range(4)]
        below_scr = refs.pop(0) if spread else None
        t = out_ref.shape[-1]
    else:
        field_ref, amp_ref = refs.pop(0), refs.pop(0)
        out_ref, sorted_ref, amp_scr, perm_scr, local_sem = [refs.pop(0) for _ in range(5)]
        t = field_ref.shape[-1]
    send_sem, recv_sem = refs
    chunk = t // PARTS
    r, c = lax.axis_index("row"), lax.axis_index("col")
    has_up, has_down = r > 0, r < rows_of - 1
    has_left, has_right = c > 0, c < cols_of - 1
    up = (jnp.where(has_up, r - 1, r + 1), c)
    down = (jnp.where(has_down, r + 1, r - 1), c)
    left = (r, jnp.where(has_left, c - 1, c + 1))
    right = (r, jnp.where(has_right, c + 1, c - 1))

    if not reduce:
        own = pltpu.make_async_copy(field_ref, out_ref.at[0, :, pl.ds(0, t)], local_sem.at[0])
        own.start()
        measured = pltpu.make_async_copy(amp_ref, amp_scr, local_sem.at[1])
        measured.start()

    barrier = pltpu.get_barrier_semaphore()
    for there, device in ((has_up, up), (has_down, down), (has_left, left), (has_right, right)):

        @pl.when(there)
        def _():
            pl.semaphore_signal(
                barrier, inc=1, device_id=device, device_id_type=pl.DeviceIdType.MESH
            )

    peers = sum(jnp.where(there, 1, 0) for there in (has_up, has_down, has_left, has_right))
    pl.semaphore_wait(barrier, peers)

    def copy(kind, i):
        rows = pl.ds(i * chunk, chunk)
        low = pl.ds(t + i * chunk, chunk)
        if kind == RIGHT_LOW:
            src, dst, device = tot_ref.at[1, :, low], side_scr.at[:, low], right
        elif kind == RIGHT_TOP:
            src, dst, device = tot_ref.at[1, :, rows], side_scr.at[:, rows], right
        elif kind == DOWN:
            src, dst, device = low_scr.at[:, rows], above_scr.at[:, rows], down
        elif kind == UP and reduce:
            src, dst, device = top_scr.at[:, rows], below_scr.at[:, rows], up
        elif kind == UP:
            src, dst, device = field_ref.at[:, rows], out_ref.at[0, :, low], up
        elif kind == LEFT and reduce:
            src, dst, device = out_ref.at[0, :, rows], out_ref.at[1, :, rows], left
        elif kind == LEFT:
            src, dst, device = field_ref.at[:, rows], out_ref.at[1, :, rows], left
        else:
            src, dst, device = out_ref.at[0, :, low], out_ref.at[1, :, low], left
        return pltpu.make_async_remote_copy(
            src_ref=src,
            dst_ref=dst,
            send_sem=send_sem.at[kind, i],
            recv_sem=recv_sem.at[kind, i],
            device_id=device,
            device_id_type=pl.DeviceIdType.MESH,
        )

    def start(there, kind, i):
        @pl.when(there)
        def _():
            copy(kind, i).start()

    def got(there, kind, i):
        @pl.when(there)
        def _():
            copy(kind, i).wait_recv()

    def sent(there, kind):
        @pl.when(there)
        def _():
            for i in range(PARTS):
                copy(kind, i).wait_send()

    if reduce:
        for i in range(PARTS):
            start(has_right, RIGHT_LOW, i)
            if spread:
                start(has_right, RIGHT_TOP, i)
        if not spread:
            for i in range(PARTS):
                start(has_right, RIGHT_TOP, i)

        @pl.when(jnp.logical_not(has_left))
        def _():
            side_scr[...] = jnp.zeros_like(side_scr)

        @pl.when(jnp.logical_not(has_up))
        def _():
            above_scr[...] = jnp.zeros_like(above_scr)

    if spread:

        @pl.when(jnp.logical_not(has_down))
        def _():
            out_ref[0, :, t:] = jnp.zeros((2, t, t), jnp.float32)

        @pl.when(jnp.logical_not(has_right))
        def _():
            out_ref[1] = jnp.zeros((2, 2 * t, t), jnp.float32)

        @pl.when(jnp.logical_and(has_right, jnp.logical_not(has_down)))
        def _():
            out_ref[1, :, t:] = jnp.zeros((2, t, t), jnp.float32)

    def band(i):
        return slice(i * chunk, (i + 1) * chunk), slice(t + i * chunk, t + (i + 1) * chunk)

    both = jnp.logical_and(has_down, has_left)
    if reduce:
        for i in range(PARTS):
            rows, low = band(i)
            got(has_left, RIGHT_LOW, i)

            @pl.when(has_down)
            def _():
                low_scr[:, rows] = tot_ref[0, :, low] + side_scr[:, low]
                copy(DOWN, i).start()

            if spread:
                got(has_left, RIGHT_TOP, i)
                top_scr[:, rows] = tot_ref[0, :, rows] + side_scr[:, rows]
                start(has_up, UP, i)
        for i in range(PARTS):
            rows, low = band(i)
            if spread:
                got(has_up, DOWN, i)
                out_ref[0, :, rows] = ext_ref[0, :, rows] - step_size * (
                    top_scr[:, rows] + above_scr[:, rows]
                )
                start(has_left, LEFT, i)

                @pl.when(has_down)
                def _():
                    copy(UP, i).wait_recv()
                    out_ref[0, :, low] = ext_ref[0, :, low] - step_size * (
                        low_scr[:, rows] + below_scr[:, rows]
                    )

                start(both, LEFT_LOW, i)
            else:
                got(has_left, RIGHT_TOP, i)
                got(has_up, DOWN, i)
                out_ref[:, rows] = ext_ref[0, :, rows] - step_size * (
                    (tot_ref[0, :, rows] + side_scr[:, rows]) + above_scr[:, rows]
                )
    else:
        for i in range(PARTS):
            start(has_up, UP, i)
            start(has_left, LEFT, i)
        spot = lax.broadcasted_iota(jnp.int32, (t, t), 1)
        spot = jnp.where(spot < t // 2, 2 * spot, 2 * spot - (t - 1))
        perm = jnp.where(lax.broadcasted_iota(jnp.int32, (t, t), 0) == spot, 1.0, 0.0)
        perm_scr[0] = perm.astype(jnp.bfloat16)
        spot = lax.broadcasted_iota(jnp.int32, (t, t), 0)
        spot = jnp.where(spot < t // 2, 2 * spot, 2 * spot - (t - 1))
        perm = jnp.where(lax.broadcasted_iota(jnp.int32, (t, t), 1) == spot, 1.0, 0.0)
        perm_scr[1] = perm.astype(jnp.bfloat16)
        measured.wait()
        slots = amp_ref.shape[0]
        done = 0
        for i in range(PARTS):
            until = min(slots, -(-slots * (i + 1) // PARTS))

            def one(s, carry):
                cols = exact(amp_scr[s], lambda piece: dot(piece, perm_scr[0]))
                sorted_ref[s] = exact(cols, lambda piece: dot(perm_scr[1], piece))
                return carry

            lax.fori_loop(done, until, one, 0)
            done = until
            got(has_down, UP, i)
            start(both, LEFT_LOW, i)
    if not reduce:
        own.wait()
    if spread:
        for i in range(PARTS):
            got(has_right, LEFT, i)
            got(jnp.logical_and(has_right, has_down), LEFT_LOW, i)
    if reduce:
        sent(has_right, RIGHT_LOW)
        sent(has_right, RIGHT_TOP)
        sent(has_down, DOWN)
    if spread:
        sent(has_up, UP)
        sent(has_left, LEFT)
        sent(both, LEFT_LOW)


def exchange(mode, *operands):
    planes, t = operands[0].shape[-3], operands[0].shape[-1]
    vmem = pl.BlockSpec(memory_space=pltpu.VMEM)
    tile = jax.ShapeDtypeStruct((planes, t, t), jnp.float32)
    shapes = [tile if mode == "reduce" else jax.ShapeDtypeStruct((2, planes, 2 * t, t), jnp.float32)]
    specs = [vmem] * len(operands)
    if mode == "spread":
        amp = operands[1]
        specs = [pl.BlockSpec(memory_space=pltpu.HBM)] * 2
        shapes.append(jax.ShapeDtypeStruct(amp.shape, jnp.float32))
        scratch = [
            pltpu.VMEM(amp.shape, jnp.float32),
            pltpu.VMEM((2, t, t), jnp.bfloat16),
            pltpu.SemaphoreType.DMA((2,)),
        ]
    else:
        scratch = [pltpu.VMEM((planes, 2 * t, t), jnp.float32)]
        scratch += [pltpu.VMEM((planes, t, t), jnp.float32)] * (4 if mode == "both" else 3)
    scratch += [pltpu.SemaphoreType.DMA((6, PARTS))] * 2
    kernel = functools.partial(
        exchange_kernel, mode, lax.axis_size("row"), lax.axis_size("col")
    )
    return pl.pallas_call(
        kernel,
        out_shape=shapes,
        in_specs=specs,
        out_specs=[vmem] * len(shapes),
        scratch_shapes=scratch,
        compiler_params=pltpu.CompilerParams(
            collective_id=("spread", "both", "reduce").index(mode),
            has_side_effects=True,
            vmem_limit_bytes=24 * 1024 * 1024,
        ),
        name="exchange_" + mode,
    )(*operands)


def tables(width):
    half = width // 2
    ladder = np.arange(width)
    theta = (ladder[:, None] * ladder[None, :] % width) * (2.0 * math.pi / width)
    factor = 1.0 / math.sqrt(width)
    cosine = np.cos(theta) * factor
    sine = np.sin(theta) * factor
    out = []
    for parity in (0, 1):
        c = cosine[parity::2, :half]
        s = sine[parity::2, :half]
        out.append(np.block([[c, s], [-s, c]]))
    stacked = np.stack(out).astype(np.float32)
    fwd = jnp.asarray(stacked).astype(jnp.bfloat16)
    inv = jnp.asarray(np.ascontiguousarray(stacked.transpose(0, 2, 1))).astype(jnp.bfloat16)
    return fwd, inv


def dot(a, b):
    return jnp.dot(a, b, preferred_element_type=jnp.float32)


ROWS_OF_CHUNK = 32


def interleave(first, second):
    out, total = [], len(first) + len(second)
    i = j = 0
    for _ in range(total):
        if j >= len(second) or (i < len(first) and i * len(second) <= j * len(first)):
            out.append(first[i])
            i += 1
        else:
            out.append(second[j])
            j += 1
    return out


class Chunks:
    def __init__(self, refs):
        self.free = [list(refs[0]), list(refs[1])]
        self.held = {}

    def feed(self, unit, key, lhs, staged=None):
        ref = self.free[unit].pop(0)
        self.held[unit, key] = ref
        pltpu.matmul_acc_lhs(ref, lhs, load_staged_rhs=staged)

    def pop(self, unit, key):
        ref = self.held.pop((unit, key))
        self.free[unit].append(ref)
        return pltpu.matmul_pop(ref)


class Step:
    def __init__(self, refs, acc):
        self.__dict__.update(refs)
        self.acc = acc
        self.modes, _, self.width, _ = self.probe.shape
        self.h = self.width // 2
        self.flip = 0

    def corner(self, s):
        lane, sub = 128, 8
        top, left = self.pos[0, s], self.pos[1, s]
        base = left // lane
        rest = left - base * lane
        over = pl.multiple_of((top // sub) * sub, sub)
        return base, rest, over, top - over

    def block_of(self, base, c):
        lane = 128
        per = self.width // lane
        half = (base + c) // per
        near = base + c - half * per
        return half, pl.ds(pl.multiple_of(near * lane, lane), lane)

    def cut_patch(self, s):
        lane, sub, width = 128, 8, self.width
        base, rest, over, drop = self.corner(s)
        part = 64
        units = []
        lanes = lax.broadcasted_iota(jnp.int32, (part, lane), 1)
        ledge = lax.broadcasted_iota(jnp.int32, (part // sub, sub, lane), 1)

        def unit(d, r):
            turned = []
            for c in range(width // lane + 1):
                half, cols = self.block_of(base, c)
                rows = pl.ds(pl.multiple_of(over + r, sub), part + sub)
                x = self.ext[half, d, rows, cols].reshape(part // sub + 1, sub, lane)
                x = pltpu.roll(x, lax.rem(sub - drop, sub), 1)
                x = jnp.where(ledge + drop < sub, x[:-1], x[1:]).reshape(part, lane)
                turned.append(pltpu.roll(x, lax.rem(lane - rest, lane), 1))
            for c in range(width // lane):
                self.patch[d, r : r + part, c * lane : (c + 1) * lane] = jnp.where(
                    lanes + rest < lane, turned[c], turned[c + 1]
                )

        for r in range(0, width, part):
            for d in range(2):
                units.append(functools.partial(unit, d, r))
        return units

    def make_psi(self, m):
        h, step = self.h, 16
        out = self.psi.at[m % 2]

        def unit(r):
            rows, low = slice(r, r + step), slice(h + r, h + r + step)
            pr, pi = self.probe[m, 0, rows], self.probe[m, 1, rows]
            qr, qi = self.probe[m, 0, low], self.probe[m, 1, low]
            fr, fi = self.patch[0, rows], self.patch[1, rows]
            gr, gi = self.patch[0, low], self.patch[1, low]
            ur, ui = pr * fr - pi * fi, pr * fi + pi * fr
            vr, vi = qr * gr - qi * gi, qr * gi + qi * gr
            out[0, rows] = (ur + vr).astype(jnp.bfloat16)
            out[0, low] = (ui + vi).astype(jnp.bfloat16)
            out[1, rows] = (ur - vr).astype(jnp.bfloat16)
            out[1, low] = (ui - vi).astype(jnp.bfloat16)

        return [functools.partial(unit, r) for r in range(0, h, step)]

    def weigh(self, m, s):
        n, h = ROWS_OF_CHUNK, self.h

        def unit(q, r):
            rows = slice(r, r + n)
            far = self.acc.pop(q, ("R1", m, r))
            self.far[m, q, rows] = far
            re, im = far[:, :h], far[:, h:]
            term = re * re + im * im
            if m > 0:
                term = self.bright[q, rows] + term
            if m < self.modes - 1:
                self.bright[q, rows] = term
            else:
                seen = self.amp[s, rows, q * h : (q + 1) * h]
                self.ratio[q, rows] = 1.0 - seen * lax.rsqrt(term + damping)

        return [functools.partial(unit, q, r) for r in range(0, self.width, n) for q in range(2)]

    def make_chi(self, m):
        n, h = ROWS_OF_CHUNK, self.h
        out = self.chi.at[m % 2]

        def unit(p, r):
            for q in range(2):
                cols = slice(q * h, (q + 1) * h)
                rows = slice(p * h + r, p * h + r + n)
                ratio = self.ratio[q, rows]
                out[p, r : r + n, cols] = (self.far[m, q, rows, :h] * ratio).astype(jnp.bfloat16)
                out[p, h + r : h + r + n, cols] = (self.far[m, q, rows, h:] * ratio).astype(
                    jnp.bfloat16
                )

        return [functools.partial(unit, p, r) for r in range(0, h, n) for p in range(2)]

    def gather(self, m):
        n, h = ROWS_OF_CHUNK, self.h

        def unit(r):
            rows = slice(r, r + n)
            even, odd = self.acc.pop(0, ("R2", m, r)), self.acc.pop(1, ("R2", m, r))
            for cols, wave in ((slice(0, h), even + odd), (slice(h, 2 * h), even - odd)):
                wr, wi = wave[:, :h], wave[:, h:]
                pr, pi = self.probe[m, 0, rows, cols], self.probe[m, 1, rows, cols]
                gr, gi = pr * wr + pi * wi, pr * wi - pi * wr
                if m > 0:
                    gr, gi = self.grad[0, rows, cols] + gr, self.grad[1, rows, cols] + gi
                self.grad[0, rows, cols] = gr
                self.grad[1, rows, cols] = gi

        return [functools.partial(unit, r) for r in range(0, self.width, n)]

    def place(self, s):
        lane, sub, width = 128, 8, self.width
        base, rest, over, drop = self.corner(s)
        wide = width // lane + 1
        blocks = width // sub
        part = 64
        lanes = lax.broadcasted_iota(jnp.int32, (part, lane), 1)

        def unit(d, r):
            edge = jnp.zeros((part, lane), jnp.float32)
            turned = [edge]
            for c in range(width // lane):
                x = self.grad[d, r : r + part, c * lane : (c + 1) * lane]
                turned.append(pltpu.roll(x, rest, 1))
            turned.append(edge)
            for c in range(wide):
                x = jnp.where(lanes >= rest, turned[c + 1], turned[c])
                x = pltpu.roll(x.reshape(part // sub, sub, lane), drop, 1)
                brim = jnp.zeros((1, sub, lane), jnp.float32)
                after = jnp.concatenate([x, brim], axis=0)
                before = jnp.concatenate([brim, x], axis=0)
                rim = lax.broadcasted_iota(jnp.int32, (part // sub + 1, sub, lane), 1)
                x = jnp.where(rim >= drop, after, before).reshape(part + sub, lane)
                half, cols = self.block_of(base, c)
                spot = (half, d, pl.ds(pl.multiple_of(over + r, sub), part + sub), cols)
                self.tot[spot] = self.tot[spot] + x

        return [functools.partial(unit, d, r) for r in range(0, width, part) for d in range(2)]

    def left(self, kind, m):
        n, h = ROWS_OF_CHUNK, self.h
        rhs, lhs = (self.psi, self.a) if kind == "L1" else (self.chi, self.b)
        reg = self.flip
        self.flip = 1 - reg

        def push():
            for unit in range(2):
                pltpu.matmul_push_rhs(rhs[m % 2, unit], reg, unit)

        def feed(r, first):
            for unit in range(2):
                self.acc.feed(unit, (kind, m, r), lhs[unit, r : r + n], reg if first else None)

        order = [r + d for r in range(0, h, n) for d in (0, h)]
        return push, [functools.partial(feed, r, k == 0) for k, r in enumerate(order)]

    def right(self, kind, m):
        n, h = ROWS_OF_CHUNK, self.h
        rhs = self.b if kind == "R1" else self.a
        reg = self.flip
        self.flip = 1 - reg

        def push():
            for unit in range(2):
                pltpu.matmul_push_rhs(rhs[unit], reg, unit)

        def feed_forward(r, p, first):
            re, im = self.acc.pop(p, ("L1", m, r)), self.acc.pop(p, ("L1", m, h + r))
            re_l, re_r, im_l, im_r = re[:, :h], re[:, h:], im[:, :h], im[:, h:]
            plus = jnp.concatenate([re_l + re_r, im_l + im_r], axis=1).astype(jnp.bfloat16)
            less = jnp.concatenate([re_l - re_r, im_l - im_r], axis=1).astype(jnp.bfloat16)
            for unit, x in enumerate((plus, less)):
                self.acc.feed(unit, (kind, m, p * h + r), x, reg if first else None)

        def feed_backward(r, first):
            key = ("L2", m, r), ("L2", m, h + r)
            ere, oim = self.acc.pop(0, key[0]), self.acc.pop(1, key[1])
            ore, eim = self.acc.pop(1, key[0]), self.acc.pop(0, key[1])
            for k, (re, im) in enumerate(((ere + ore, eim + oim), (ere - ore, eim - oim))):
                for unit in range(2):
                    cols = slice(unit * h, (unit + 1) * h)
                    y = jnp.concatenate([re[:, cols], im[:, cols]], axis=1).astype(jnp.bfloat16)
                    self.acc.feed(
                        unit, (kind, m, k * h + r), y, reg if first and k == 0 else None
                    )

        if kind == "R1":
            spots = [(r, p) for r in range(0, h, n) for p in range(2)]
            feeds = [functools.partial(feed_forward, r, p, k == 0) for k, (r, p) in enumerate(spots)]
        else:
            feeds = [functools.partial(feed_backward, r, r == 0) for r in range(0, h, n)]
        return push, feeds

    def run(self, jobs):
        built = []
        for kind, m, beside in jobs:
            if kind is None:
                built.append((None, [], beside))
                continue
            push, feeds = (self.left if kind[0] == "L" else self.right)(kind, m)
            built.append((push, feeds, beside))
        for k, (push, feeds, beside) in enumerate(built):
            if push is not None and (k == 0 or built[k - 1][0] is None):
                push()
            for unit in interleave(feeds, beside):
                unit()
            if push is not None and k + 1 < len(built) and built[k + 1][0] is not None:
                built[k + 1][0]()


def forward_only(step, s, ahead, ready):
    psi, weigh = step.make_psi, lambda m: step.weigh(m, s)
    for unit in step.cut_patch(s) + psi(0) + psi(1):
        unit()
    ready()
    step.run(
        [
            ("L1", 0, []),
            ("L1", 1, psi(2)),
            ("R1", 0, psi(3)),
            ("L1", 2, weigh(0)),
            ("R1", 1, step.cut_patch(ahead)),
            ("L1", 3, weigh(1)),
            ("R1", 2, psi(0)),
            ("R1", 3, weigh(2)),
            (None, 0, weigh(3)),
        ]
    )


def backward_only(step, s, behind):
    chi, gather, place = step.make_chi, step.gather, step.place(behind)
    half = len(place) // 2
    step.run(
        [
            (None, 0, chi(0)),
            ("L2", 0, chi(1) + place[:half]),
            ("L2", 1, chi(2) + place[half:]),
            ("R2", 0, []),
            ("L2", 2, chi(3) + gather(0)),
            ("R2", 1, []),
            ("L2", 3, gather(1)),
            ("R2", 2, []),
            ("R2", 3, gather(2)),
            (None, 0, gather(3) + step.place(s)),
        ]
    )


def both_ways(step, behind, back, ahead, beyond):
    psi, weigh = step.make_psi, lambda m: step.weigh(m, ahead)
    chi, gather = step.make_chi, step.gather
    cut, place = step.cut_patch(beyond), step.place(behind)
    psi1, psi2, psi3 = psi(1), psi(2), psi(3)
    g0, g1, g2 = gather(0), gather(1), gather(2)
    step.run(
        [
            ("L1", 0, chi(0) + psi1[:4]),
            ("L2", 0, psi1[4:] + place[:3]),
            ("L1", 1, chi(1) + place[3:6]),
            ("R1", 0, place[6:] + psi2[:2]),
            ("R2", 0, psi2[2:7]),
            ("L2", 1, psi2[7:] + weigh(0)),
            ("L1", 2, interleave(g0, chi(2))),
            ("R1", 1, psi3[:5]),
            ("R2", 1, psi3[5:]),
            ("L2", 2, weigh(1) + g1[:4]),
            ("L1", 3, interleave(g1[4:], chi(3))),
            ("R1", 2, cut[:5]),
            ("R2", 2, cut[5:]),
            ("L2", 3, weigh(2) + psi(0)[:0]),
            ("R1", 3, g2 + psi(0)[:4]),
            ("R2", 3, psi(0)[4:] + weigh(3)),
            (None, 0, gather(3)),
        ]
    )


NAMES = ("count", "pos", "ext", "amp", "probe", "a_hbm", "b_hbm", "tot")
NAMES += ("patch", "psi", "far", "chi", "grad", "bright", "ratio", "a", "b", "sem")


def gradient_kernel(*operands):
    refs = dict(zip(NAMES, operands))
    sem = refs["sem"]
    fetch = [
        pltpu.make_async_copy(refs[name + "_hbm"], refs[name], sem.at[k])
        for k, name in enumerate("ab")
    ]
    for copy in fetch:
        copy.start()
    refs["tot"][...] = jnp.zeros_like(refs["tot"])
    refs["grad"][...] = jnp.zeros_like(refs["grad"])
    count = refs["count"][0, 0]
    last = refs["amp"].shape[0] - 1

    def with_units(work, *where):
        def body(*acc):
            half = len(acc) // 2
            work(Step(refs, Chunks((acc[:half], acc[half:]))), *where)

        depth = 1024 // ROWS_OF_CHUNK
        shape = (ROWS_OF_CHUNK, refs["probe"].shape[-1])
        pl.run_scoped(body, *[pltpu.ACC(u)(shape, jnp.float32) for u in (0, 1) for _ in range(depth)])

    def ready():
        for copy in fetch:
            copy.wait()

    @pl.when(count > 0)
    def _():
        with_units(forward_only, 0, min(1, last), ready)

    @pl.when(count <= 0)
    def _():
        ready()

    def one(s, carry):
        with_units(both_ways, jnp.maximum(s - 1, 0), s, s + 1, jnp.minimum(s + 2, last))
        return carry

    lax.fori_loop(0, count - 1, one, 0)

    @pl.when(count > 0)
    def _():
        with_units(backward_only, count - 1, jnp.maximum(count - 2, 0))


def gradient(counts, where, extended, amp, probe_modes, fwd, inv):
    modes, _, width, _ = probe_modes.shape
    vmem = pl.BlockSpec(memory_space=pltpu.VMEM)
    smem = pl.BlockSpec(memory_space=pltpu.SMEM)
    hbm = pl.BlockSpec(memory_space=pltpu.HBM)
    half = width // 2
    return pl.pallas_call(
        gradient_kernel,
        out_shape=jax.ShapeDtypeStruct(extended.shape, jnp.float32),
        in_specs=[smem, smem] + [vmem] * 3 + [hbm] * 2,
        out_specs=vmem,
        scratch_shapes=[
            pltpu.VMEM((2, width, width), jnp.float32),
            pltpu.VMEM((2, 2, width, width), jnp.bfloat16),
            pltpu.VMEM((modes, 2, width, width), jnp.float32),
            pltpu.VMEM((2, 2, width, width), jnp.bfloat16),
            pltpu.VMEM((2, width, width), jnp.float32),
            pltpu.VMEM((2, width, half), jnp.float32),
            pltpu.VMEM((2, width, half), jnp.float32),
            pltpu.VMEM(fwd.shape, jnp.bfloat16),
            pltpu.VMEM(inv.shape, jnp.bfloat16),
            pltpu.SemaphoreType.DMA((2,)),
        ],
        compiler_params=pltpu.CompilerParams(vmem_limit_bytes=40 * 1024 * 1024),
        name="gradient",
    )(counts, where, extended, amp, probe_modes, fwd, inv)


def exact(values, product):
    total = None
    for _ in range(3):
        piece = values.astype(jnp.bfloat16)
        values = values - piece.astype(jnp.float32)
        part = product(piece)
        total = part if total is None else total + part
    return total


def body(object_field, probe_modes, positions, counts, amplitude):
    width = probe_modes.shape[-1]
    fwd, inv = [pltpu.with_memory_space_constraint(x, pltpu.HBM) for x in tables(width)]
    where = positions[0, 0].T
    held = [pltpu.with_memory_space_constraint(x, pltpu.HBM) for x in (object_field, amplitude[0, 0])]
    extended, amp = exchange("spread", *held)
    for sweep in range(ITERS):
        total = gradient(counts, where, extended, amp, probe_modes, fwd, inv)
        (extended,) = exchange("both" if sweep < ITERS - 1 else "reduce", total, extended)
    return extended


def solution(mesh):
    placed = (
        P(None, "row", "col"),
        P(),
        P("row", "col", None, None),
        P("row", "col"),
        P("row", "col", None, None, None),
    )
    return jax.shard_map(
        body, mesh=mesh, in_specs=placed, out_specs=P(None, "row", "col"), check_vma=False
    )
```

```python
import functools
import math

import jax
import jax.numpy as jnp
import numpy as np
from jax import lax
from jax.experimental import pallas as pl
from jax.experimental.pallas import tpu as pltpu
from jax.sharding import PartitionSpec as P

ITERS = 2


step_size = 0.1
damping = 0.1


RIGHT_LOW, RIGHT_TOP, DOWN, UP, LEFT, LEFT_LOW = range(6)
UP_VIA, UP_ON, DOWN_VIA, DOWN_ON = range(6, 10)
PARTS = 4


def exchange_kernel(mode, rows_of, cols_of, *refs):
    refs = list(refs)
    reduce, spread = mode != "spread", mode != "reduce"
    if reduce:
        tot_ref, ext_ref, out_ref = refs.pop(0), refs.pop(0), refs.pop(0)
        side_scr, top_scr, low_scr, above_scr = [refs.pop(0) for _ in range(4)]
        below_scr = refs.pop(0) if spread else None
        via_scr = refs.pop(0) if spread else None
        t = out_ref.shape[-1]
    else:
        field_ref, amp_ref = refs.pop(0), refs.pop(0)
        out_ref, sorted_ref, amp_scr, perm_scr, local_sem = [refs.pop(0) for _ in range(5)]
        t = field_ref.shape[-1]
    send_sem, recv_sem = refs
    chunk = t // PARTS
    r, c = lax.axis_index("row"), lax.axis_index("col")
    has_up, has_down = r > 0, r < rows_of - 1
    has_left, has_right = c > 0, c < cols_of - 1
    up = (jnp.where(has_up, r - 1, r + 1), c)
    down = (jnp.where(has_down, r + 1, r - 1), c)
    left = (r, jnp.where(has_left, c - 1, c + 1))
    right = (r, jnp.where(has_right, c + 1, c - 1))
    folded = reduce and spread and rows_of % 2 == 0 and rows_of > 2
    even, odd = lax.rem(r, 2) == 0, lax.rem(r, 2) == 1
    has_up2, has_down2 = r > 1, r < rows_of - 2
    up2 = (jnp.where(has_up2, r - 2, r + 2), c)
    down2 = (jnp.where(has_down2, r + 2, r - 2), c)
    far_up, far_down = jnp.logical_and(even, has_up), jnp.logical_and(odd, has_down)
    relay_up, relay_down = jnp.logical_and(even, has_down2), jnp.logical_and(odd, has_up2)

    def goes_round(i):
        return folded and i % 2 == 0

    def but(a, b):
        return jnp.logical_and(a, jnp.logical_not(b))

    if not reduce:
        own = pltpu.make_async_copy(field_ref, out_ref.at[0, :, pl.ds(0, t)], local_sem.at[0])
        own.start()
        measured = pltpu.make_async_copy(amp_ref, amp_scr, local_sem.at[1])
        measured.start()

    barrier = pltpu.get_barrier_semaphore()
    peers_of = [(has_up, up), (has_down, down), (has_left, left), (has_right, right)]
    if folded:
        peers_of += [(has_up2, up2), (has_down2, down2)]
    for there, device in peers_of:

        @pl.when(there)
        def _():
            pl.semaphore_signal(
                barrier, inc=1, device_id=device, device_id_type=pl.DeviceIdType.MESH
            )

    peers = sum(jnp.where(there, 1, 0) for there, _ in peers_of)
    pl.semaphore_wait(barrier, peers)

    def copy(kind, i):
        rows = pl.ds(i * chunk, chunk)
        low = pl.ds(t + i * chunk, chunk)
        if kind == RIGHT_LOW:
            src, dst, device = tot_ref.at[1, :, low], side_scr.at[:, low], right
        elif kind == RIGHT_TOP:
            src, dst, device = tot_ref.at[1, :, rows], side_scr.at[:, rows], right
        elif kind == DOWN:
            src, dst, device = low_scr.at[:, rows], above_scr.at[:, rows], down
        elif kind == UP and reduce:
            src, dst, device = top_scr.at[:, rows], below_scr.at[:, rows], up
        elif kind == UP:
            src, dst, device = field_ref.at[:, rows], out_ref.at[0, :, low], up
        elif kind == UP_VIA:
            src, dst, device = top_scr.at[:, rows], via_scr.at[:, rows], up2
        elif kind == UP_ON:
            src, dst, device = via_scr.at[:, rows], below_scr.at[:, rows], down
        elif kind == DOWN_VIA:
            src, dst, device = low_scr.at[:, rows], via_scr.at[:, rows], down2
        elif kind == DOWN_ON:
            src, dst, device = via_scr.at[:, rows], above_scr.at[:, rows], up
        elif kind == LEFT and reduce:
            src, dst, device = out_ref.at[0, :, rows], out_ref.at[1, :, rows], left
        elif kind == LEFT:
            src, dst, device = field_ref.at[:, rows], out_ref.at[1, :, rows], left
        else:
            src, dst, device = out_ref.at[0, :, low], out_ref.at[1, :, low], left
        return pltpu.make_async_remote_copy(
            src_ref=src,
            dst_ref=dst,
            send_sem=send_sem.at[kind, i],
            recv_sem=recv_sem.at[kind, i],
            device_id=device,
            device_id_type=pl.DeviceIdType.MESH,
        )

    def start(there, kind, i):
        @pl.when(there)
        def _():
            copy(kind, i).start()

    def got(there, kind, i):
        @pl.when(there)
        def _():
            copy(kind, i).wait_recv()

    def sent(there, kind, parts=range(PARTS)):
        @pl.when(there)
        def _():
            for i in parts:
                copy(kind, i).wait_send()

    if reduce:
        for i in range(PARTS):
            start(jnp.logical_and(has_right, even) if spread else has_right, RIGHT_LOW, i)
            if spread:
                start(has_right, RIGHT_TOP, i)
                start(jnp.logical_and(has_right, odd), RIGHT_LOW, i)
        if not spread:
            for i in range(PARTS):
                start(has_right, RIGHT_TOP, i)

        @pl.when(jnp.logical_not(has_left))
        def _():
            side_scr[...] = jnp.zeros_like(side_scr)

        @pl.when(jnp.logical_not(has_up))
        def _():
            above_scr[...] = jnp.zeros_like(above_scr)

    if spread:

        @pl.when(jnp.logical_not(has_down))
        def _():
            out_ref[0, :, t:] = jnp.zeros((2, t, t), jnp.float32)

        @pl.when(jnp.logical_not(has_right))
        def _():
            out_ref[1] = jnp.zeros((2, 2 * t, t), jnp.float32)

        @pl.when(jnp.logical_and(has_right, jnp.logical_not(has_down)))
        def _():
            out_ref[1, :, t:] = jnp.zeros((2, t, t), jnp.float32)

    def band(i):
        return slice(i * chunk, (i + 1) * chunk), slice(t + i * chunk, t + (i + 1) * chunk)

    both = jnp.logical_and(has_down, has_left)
    if reduce:
        def ready(i):
            rows, low = band(i)
            got(has_left, RIGHT_LOW, i)

            @pl.when(has_down)
            def _():
                low_scr[:, rows] = tot_ref[0, :, low] + side_scr[:, low]

            if spread:
                got(has_left, RIGHT_TOP, i)
                top_scr[:, rows] = tot_ref[0, :, rows] + side_scr[:, rows]

        def within(i):
            start(jnp.logical_and(odd, has_up), UP, i)
            start(jnp.logical_and(even, has_down), DOWN, i)

        def across(i):
            start(far_up, UP_VIA if goes_round(i) else UP, i)
            start(far_down, DOWN_VIA if goes_round(i) else DOWN, i)

        def pass_on(i):
            got(relay_up, UP_VIA, i)
            start(relay_up, UP_ON, i)
            got(relay_down, DOWN_VIA, i)
            start(relay_down, DOWN_ON, i)

        def own_band(there, i, kinds):
            rows, _ = band(i)

            @pl.when(there)
            def _():
                for also, kind in kinds:
                    got(also, kind, i)
                out_ref[0, :, rows] = ext_ref[0, :, rows] - step_size * (
                    top_scr[:, rows] + above_scr[:, rows]
                )
                start(has_left, LEFT, i)

        def low_band(there, i, kinds):
            rows, low = band(i)

            @pl.when(jnp.logical_and(there, has_down))
            def _():
                for also, kind in kinds:
                    got(also, kind, i)
                out_ref[0, :, low] = ext_ref[0, :, low] - step_size * (
                    low_scr[:, rows] + below_scr[:, rows]
                )
                start(has_left, LEFT_LOW, i)

        def settle_within(i):
            low_band(even, i, [(has_down, UP)])
            own_band(odd, i, [(has_up, DOWN)])

        def settle_across(i):
            own_band(even, i, [(has_up, DOWN_ON if goes_round(i) else DOWN)])
            low_band(odd, i, [(has_down, UP_ON if goes_round(i) else UP)])

        if spread and folded:
            for i in range(0, PARTS, 2):
                ready(i)
                if i > 0:
                    pass_on(i - 2)
                within(i)
                across(i)
                ready(i + 1)
                if i == 0:
                    within(i + 1)
                    across(i + 1)
                else:
                    across(i + 1)
                    within(i + 1)
            late = PARTS - 2
            settle_within(0)
            settle_within(1)
            pass_on(late)
            for i in range(PARTS):
                settle_across(i)
                if i > 0 and i + 1 < PARTS:
                    settle_within(i + 1)
        elif spread:
            for i in range(PARTS):
                ready(i)
                within(i)
                across(i)
            for i in range(PARTS):
                settle_within(i)
                settle_across(i)
        for i in range(PARTS):
            rows, low = band(i)
            if spread:
                continue
            ready(i)
            start(has_down, DOWN, i)
        for i in range(PARTS):
            rows, low = band(i)
            if spread:
                continue
            got(has_left, RIGHT_TOP, i)
            got(has_up, DOWN, i)
            out_ref[:, rows] = ext_ref[0, :, rows] - step_size * (
                (tot_ref[0, :, rows] + side_scr[:, rows]) + above_scr[:, rows]
            )
    else:
        for i in range(PARTS):
            start(has_up, UP, i)
            start(has_left, LEFT, i)
        spot = lax.broadcasted_iota(jnp.int32, (t, t), 1)
        spot = jnp.where(spot < t // 2, 2 * spot, 2 * spot - (t - 1))
        perm = jnp.where(lax.broadcasted_iota(jnp.int32, (t, t), 0) == spot, 1.0, 0.0)
        perm_scr[0] = perm.astype(jnp.bfloat16)
        spot = lax.broadcasted_iota(jnp.int32, (t, t), 0)
        spot = jnp.where(spot < t // 2, 2 * spot, 2 * spot - (t - 1))
        perm = jnp.where(lax.broadcasted_iota(jnp.int32, (t, t), 1) == spot, 1.0, 0.0)
        perm_scr[1] = perm.astype(jnp.bfloat16)
        measured.wait()
        slots = amp_ref.shape[0]
        done = 0
        for i in range(PARTS):
            until = min(slots, -(-slots * (i + 1) // (PARTS - 2)))

            def one(s, carry):
                cols = exact(amp_scr[s], lambda piece: dot(piece, perm_scr[0]))
                sorted_ref[s] = exact(cols, lambda piece: dot(perm_scr[1], piece))
                return carry

            lax.fori_loop(done, until, one, 0)
            done = until
            got(has_down, UP, i)
            start(both, LEFT_LOW, i)
    if not reduce:
        own.wait()
    if spread:
        for i in range(PARTS):
            got(has_right, LEFT, i)
            got(jnp.logical_and(has_right, has_down), LEFT_LOW, i)
    round_parts = [i for i in range(PARTS) if goes_round(i)]
    plain_parts = [i for i in range(PARTS) if not goes_round(i)]
    if reduce:
        sent(has_right, RIGHT_LOW)
        sent(has_right, RIGHT_TOP)
        sent(has_down, DOWN, plain_parts)
    if folded:
        sent(but(has_down, far_down), DOWN, round_parts)
        sent(far_down, DOWN_VIA, round_parts)
        sent(relay_down, DOWN_ON, round_parts)
        sent(but(has_up, far_up), UP, round_parts)
        sent(far_up, UP_VIA, round_parts)
        sent(relay_up, UP_ON, round_parts)
    if spread:
        sent(has_up, UP, plain_parts)
        sent(has_left, LEFT)
        sent(both, LEFT_LOW)


def exchange(mode, *operands):
    planes, t = operands[0].shape[-3], operands[0].shape[-1]
    vmem = pl.BlockSpec(memory_space=pltpu.VMEM)
    tile = jax.ShapeDtypeStruct((planes, t, t), jnp.float32)
    shapes = [tile if mode == "reduce" else jax.ShapeDtypeStruct((2, planes, 2 * t, t), jnp.float32)]
    specs = [vmem] * len(operands)
    if mode == "spread":
        amp = operands[1]
        specs = [pl.BlockSpec(memory_space=pltpu.HBM)] * 2
        shapes.append(jax.ShapeDtypeStruct(amp.shape, jnp.float32))
        scratch = [
            pltpu.VMEM(amp.shape, jnp.float32),
            pltpu.VMEM((2, t, t), jnp.bfloat16),
            pltpu.SemaphoreType.DMA((2,)),
        ]
    else:
        scratch = [pltpu.VMEM((planes, 2 * t, t), jnp.float32)]
        scratch += [pltpu.VMEM((planes, t, t), jnp.float32)] * (5 if mode == "both" else 3)
    scratch += [pltpu.SemaphoreType.DMA((10, PARTS))] * 2
    kernel = functools.partial(
        exchange_kernel, mode, lax.axis_size("row"), lax.axis_size("col")
    )
    return pl.pallas_call(
        kernel,
        out_shape=shapes,
        in_specs=specs,
        out_specs=[vmem] * len(shapes),
        scratch_shapes=scratch,
        compiler_params=pltpu.CompilerParams(
            collective_id=("spread", "both", "reduce").index(mode),
            has_side_effects=True,
            vmem_limit_bytes=24 * 1024 * 1024,
        ),
        name="exchange_" + mode,
    )(*operands)


def tables(width):
    half = width // 2
    ladder = np.arange(width)
    theta = (ladder[:, None] * ladder[None, :] % width) * (2.0 * math.pi / width)
    factor = 1.0 / math.sqrt(width)
    cosine = np.cos(theta) * factor
    sine = np.sin(theta) * factor
    out = []
    for parity in (0, 1):
        c = cosine[parity::2, :half]
        s = sine[parity::2, :half]
        out.append(np.block([[c, s], [-s, c]]))
    stacked = np.stack(out).astype(np.float32)
    fwd = jnp.asarray(stacked).astype(jnp.bfloat16)
    inv = jnp.asarray(np.ascontiguousarray(stacked.transpose(0, 2, 1))).astype(jnp.bfloat16)
    return fwd, inv


def dot(a, b):
    return jnp.dot(a, b, preferred_element_type=jnp.float32)


ROWS_OF_CHUNK = 32


def interleave(first, second):
    out, total = [], len(first) + len(second)
    i = j = 0
    for _ in range(total):
        if j >= len(second) or (i < len(first) and i * len(second) <= j * len(first)):
            out.append(first[i])
            i += 1
        else:
            out.append(second[j])
            j += 1
    return out


class Chunks:
    def __init__(self, refs):
        self.free = [list(refs[0]), list(refs[1])]
        self.held = {}

    def feed(self, unit, key, lhs, staged=None):
        ref = self.free[unit].pop(0)
        self.held[unit, key] = ref
        pltpu.matmul_acc_lhs(ref, lhs, load_staged_rhs=staged)

    def pop(self, unit, key):
        ref = self.held.pop((unit, key))
        self.free[unit].append(ref)
        return pltpu.matmul_pop(ref)


class Step:
    def __init__(self, refs, acc):
        self.__dict__.update(refs)
        self.acc = acc
        self.modes, _, self.width, _ = self.probe.shape
        self.h = self.width // 2
        self.flip = 0

    def corner(self, s):
        lane, sub = 128, 8
        top, left = self.pos[0, s], self.pos[1, s]
        base = left // lane
        rest = left - base * lane
        over = pl.multiple_of((top // sub) * sub, sub)
        return base, rest, over, top - over

    def block_of(self, base, c):
        lane = 128
        per = self.width // lane
        half = (base + c) // per
        near = base + c - half * per
        return half, pl.ds(pl.multiple_of(near * lane, lane), lane)

    def cut_patch(self, s):
        lane, sub, width = 128, 8, self.width
        base, rest, over, drop = self.corner(s)
        part = 64
        units = []
        lanes = lax.broadcasted_iota(jnp.int32, (part, lane), 1)
        ledge = lax.broadcasted_iota(jnp.int32, (part // sub, sub, lane), 1)

        def unit(d, r):
            turned = []
            for c in range(width // lane + 1):
                half, cols = self.block_of(base, c)
                rows = pl.ds(pl.multiple_of(over + r, sub), part + sub)
                x = self.ext[half, d, rows, cols].reshape(part // sub + 1, sub, lane)
                x = pltpu.roll(x, lax.rem(sub - drop, sub), 1)
                x = jnp.where(ledge + drop < sub, x[:-1], x[1:]).reshape(part, lane)
                turned.append(pltpu.roll(x, lax.rem(lane - rest, lane), 1))
            for c in range(width // lane):
                self.patch[d, r : r + part, c * lane : (c + 1) * lane] = jnp.where(
                    lanes + rest < lane, turned[c], turned[c + 1]
                )

        for r in range(0, width, part):
            for d in range(2):
                units.append(functools.partial(unit, d, r))
        return units

    def make_psi(self, m):
        h, step = self.h, 16
        out = self.psi.at[m % 2]

        def unit(r):
            rows, low = slice(r, r + step), slice(h + r, h + r + step)
            pr, pi = self.probe[m, 0, rows], self.probe[m, 1, rows]
            qr, qi = self.probe[m, 0, low], self.probe[m, 1, low]
            fr, fi = self.patch[0, rows], self.patch[1, rows]
            gr, gi = self.patch[0, low], self.patch[1, low]
            ur, ui = pr * fr - pi * fi, pr * fi + pi * fr
            vr, vi = qr * gr - qi * gi, qr * gi + qi * gr
            out[0, rows] = (ur + vr).astype(jnp.bfloat16)
            out[0, low] = (ui + vi).astype(jnp.bfloat16)
            out[1, rows] = (ur - vr).astype(jnp.bfloat16)
            out[1, low] = (ui - vi).astype(jnp.bfloat16)

        return [functools.partial(unit, r) for r in range(0, h, step)]

    def weigh(self, m, s):
        n, h = ROWS_OF_CHUNK, self.h

        def unit(q, r):
            rows = slice(r, r + n)
            far = self.acc.pop(q, ("R1", m, r))
            self.far[m, q, rows] = far
            re, im = far[:, :h], far[:, h:]
            term = re * re + im * im
            if m > 0:
                term = self.bright[q, rows] + term
            if m < self.modes - 1:
                self.bright[q, rows] = term
            else:
                seen = self.amp[s, rows, q * h : (q + 1) * h]
                self.ratio[q, rows] = 1.0 - seen * lax.rsqrt(term + damping)

        return [functools.partial(unit, q, r) for r in range(0, self.width, n) for q in range(2)]

    def make_chi(self, m):
        n, h = ROWS_OF_CHUNK, self.h
        out = self.chi.at[m % 2]

        def unit(p, r):
            for q in range(2):
                cols = slice(q * h, (q + 1) * h)
                rows = slice(p * h + r, p * h + r + n)
                ratio = self.ratio[q, rows]
                out[p, r : r + n, cols] = (self.far[m, q, rows, :h] * ratio).astype(jnp.bfloat16)
                out[p, h + r : h + r + n, cols] = (self.far[m, q, rows, h:] * ratio).astype(
                    jnp.bfloat16
                )

        return [functools.partial(unit, p, r) for r in range(0, h, n) for p in range(2)]

    def gather(self, m):
        n, h = ROWS_OF_CHUNK, self.h

        def unit(r):
            rows = slice(r, r + n)
            even, odd = self.acc.pop(0, ("R2", m, r)), self.acc.pop(1, ("R2", m, r))
            for cols, wave in ((slice(0, h), even + odd), (slice(h, 2 * h), even - odd)):
                wr, wi = wave[:, :h], wave[:, h:]
                pr, pi = self.probe[m, 0, rows, cols], self.probe[m, 1, rows, cols]
                gr, gi = pr * wr + pi * wi, pr * wi - pi * wr
                if m > 0:
                    gr, gi = self.grad[0, rows, cols] + gr, self.grad[1, rows, cols] + gi
                self.grad[0, rows, cols] = gr
                self.grad[1, rows, cols] = gi

        return [functools.partial(unit, r) for r in range(0, self.width, n)]

    def place(self, s):
        lane, sub, width = 128, 8, self.width
        base, rest, over, drop = self.corner(s)
        wide = width // lane + 1
        blocks = width // sub
        part = 64
        lanes = lax.broadcasted_iota(jnp.int32, (part, lane), 1)

        def unit(d, r):
            edge = jnp.zeros((part, lane), jnp.float32)
            turned = [edge]
            for c in range(width // lane):
                x = self.grad[d, r : r + part, c * lane : (c + 1) * lane]
                turned.append(pltpu.roll(x, rest, 1))
            turned.append(edge)
            for c in range(wide):
                x = jnp.where(lanes >= rest, turned[c + 1], turned[c])
                x = pltpu.roll(x.reshape(part // sub, sub, lane), drop, 1)
                brim = jnp.zeros((1, sub, lane), jnp.float32)
                after = jnp.concatenate([x, brim], axis=0)
                before = jnp.concatenate([brim, x], axis=0)
                rim = lax.broadcasted_iota(jnp.int32, (part // sub + 1, sub, lane), 1)
                x = jnp.where(rim >= drop, after, before).reshape(part + sub, lane)
                half, cols = self.block_of(base, c)
                spot = (half, d, pl.ds(pl.multiple_of(over + r, sub), part + sub), cols)
                self.tot[spot] = self.tot[spot] + x

        return [functools.partial(unit, d, r) for r in range(0, width, part) for d in range(2)]

    def left(self, kind, m):
        n, h = ROWS_OF_CHUNK, self.h
        rhs, lhs = (self.psi, self.a) if kind == "L1" else (self.chi, self.b)
        reg = self.flip
        self.flip = 1 - reg

        def push():
            for unit in range(2):
                pltpu.matmul_push_rhs(rhs[m % 2, unit], reg, unit)

        def feed(r, first):
            for unit in range(2):
                self.acc.feed(unit, (kind, m, r), lhs[unit, r : r + n], reg if first else None)

        order = [r + d for r in range(0, h, n) for d in (0, h)]
        return push, [functools.partial(feed, r, k == 0) for k, r in enumerate(order)]

    def right(self, kind, m):
        n, h = ROWS_OF_CHUNK, self.h
        rhs = self.b if kind == "R1" else self.a
        reg = self.flip
        self.flip = 1 - reg

        def push():
            for unit in range(2):
                pltpu.matmul_push_rhs(rhs[unit], reg, unit)

        def feed_forward(r, p, first):
            re, im = self.acc.pop(p, ("L1", m, r)), self.acc.pop(p, ("L1", m, h + r))
            re_l, re_r, im_l, im_r = re[:, :h], re[:, h:], im[:, :h], im[:, h:]
            plus = jnp.concatenate([re_l + re_r, im_l + im_r], axis=1).astype(jnp.bfloat16)
            less = jnp.concatenate([re_l - re_r, im_l - im_r], axis=1).astype(jnp.bfloat16)
            for unit, x in enumerate((plus, less)):
                self.acc.feed(unit, (kind, m, p * h + r), x, reg if first else None)

        def feed_backward(r, first):
            key = ("L2", m, r), ("L2", m, h + r)
            ere, oim = self.acc.pop(0, key[0]), self.acc.pop(1, key[1])
            ore, eim = self.acc.pop(1, key[0]), self.acc.pop(0, key[1])
            for k, (re, im) in enumerate(((ere + ore, eim + oim), (ere - ore, eim - oim))):
                for unit in range(2):
                    cols = slice(unit * h, (unit + 1) * h)
                    y = jnp.concatenate([re[:, cols], im[:, cols]], axis=1).astype(jnp.bfloat16)
                    self.acc.feed(
                        unit, (kind, m, k * h + r), y, reg if first and k == 0 else None
                    )

        if kind == "R1":
            spots = [(r, p) for r in range(0, h, n) for p in range(2)]
            feeds = [functools.partial(feed_forward, r, p, k == 0) for k, (r, p) in enumerate(spots)]
        else:
            feeds = [functools.partial(feed_backward, r, r == 0) for r in range(0, h, n)]
        return push, feeds

    def run(self, jobs):
        built = []
        for kind, m, beside in jobs:
            if kind is None:
                built.append((None, [], beside))
                continue
            push, feeds = (self.left if kind[0] == "L" else self.right)(kind, m)
            built.append((push, feeds, beside))
        for k, (push, feeds, beside) in enumerate(built):
            if push is not None and (k == 0 or built[k - 1][0] is None):
                push()
            for unit in interleave(feeds, beside):
                unit()
            if push is not None and k + 1 < len(built) and built[k + 1][0] is not None:
                built[k + 1][0]()


def forward_only(step, s, ahead, ready):
    psi, weigh = step.make_psi, lambda m: step.weigh(m, s)
    for unit in step.cut_patch(s) + psi(0) + psi(1):
        unit()
    ready()
    step.run(
        [
            ("L1", 0, []),
            ("L1", 1, psi(2)),
            ("R1", 0, psi(3)),
            ("L1", 2, weigh(0)),
            ("R1", 1, step.cut_patch(ahead)),
            ("L1", 3, weigh(1)),
            ("R1", 2, psi(0)),
            ("R1", 3, weigh(2)),
            (None, 0, weigh(3)),
        ]
    )


def backward_only(step, s, behind):
    chi, gather, place = step.make_chi, step.gather, step.place(behind)
    half = len(place) // 2
    step.run(
        [
            (None, 0, chi(0)),
            ("L2", 0, chi(1) + place[:half]),
            ("L2", 1, chi(2) + place[half:]),
            ("R2", 0, []),
            ("L2", 2, chi(3) + gather(0)),
            ("R2", 1, []),
            ("L2", 3, gather(1)),
            ("R2", 2, []),
            ("R2", 3, gather(2)),
            (None, 0, gather(3) + step.place(s)),
        ]
    )


def both_ways(step, behind, back, ahead, beyond):
    psi, weigh = step.make_psi, lambda m: step.weigh(m, ahead)
    chi, gather = step.make_chi, step.gather
    cut, place = step.cut_patch(beyond), step.place(behind)
    psi1, psi2, psi3 = psi(1), psi(2), psi(3)
    g0, g1, g2 = gather(0), gather(1), gather(2)
    step.run(
        [
            ("L1", 0, chi(0) + psi1[:4]),
            ("L2", 0, psi1[4:] + place[:3]),
            ("L1", 1, chi(1) + place[3:6]),
            ("R1", 0, place[6:] + psi2[:2]),
            ("R2", 0, psi2[2:7]),
            ("L2", 1, psi2[7:] + weigh(0)),
            ("L1", 2, interleave(g0, chi(2))),
            ("R1", 1, psi3[:5]),
            ("R2", 1, psi3[5:]),
            ("L2", 2, weigh(1) + g1[:4]),
            ("L1", 3, interleave(g1[4:], chi(3))),
            ("R1", 2, cut[:5]),
            ("R2", 2, cut[5:]),
            ("L2", 3, weigh(2) + psi(0)[:0]),
            ("R1", 3, g2 + psi(0)[:4]),
            ("R2", 3, psi(0)[4:] + weigh(3)),
            (None, 0, gather(3)),
        ]
    )


NAMES = ("count", "pos", "ext", "amp", "probe", "a_hbm", "b_hbm", "tot")
NAMES += ("patch", "psi", "far", "chi", "grad", "bright", "ratio", "a", "b", "sem")


def gradient_kernel(*operands):
    refs = dict(zip(NAMES, operands))
    sem = refs["sem"]
    fetch = [
        pltpu.make_async_copy(refs[name + "_hbm"], refs[name], sem.at[k])
        for k, name in enumerate("ab")
    ]
    for copy in fetch:
        copy.start()
    refs["tot"][...] = jnp.zeros_like(refs["tot"])
    refs["grad"][...] = jnp.zeros_like(refs["grad"])
    count = refs["count"][0, 0]
    last = refs["amp"].shape[0] - 1

    def with_units(work, *where):
        def body(*acc):
            half = len(acc) // 2
            work(Step(refs, Chunks((acc[:half], acc[half:]))), *where)

        depth = 1024 // ROWS_OF_CHUNK
        shape = (ROWS_OF_CHUNK, refs["probe"].shape[-1])
        pl.run_scoped(body, *[pltpu.ACC(u)(shape, jnp.float32) for u in (0, 1) for _ in range(depth)])

    def ready():
        for copy in fetch:
            copy.wait()

    @pl.when(count > 0)
    def _():
        with_units(forward_only, 0, min(1, last), ready)

    @pl.when(count <= 0)
    def _():
        ready()

    def one(s, carry):
        with_units(both_ways, jnp.maximum(s - 1, 0), s, s + 1, jnp.minimum(s + 2, last))
        return carry

    lax.fori_loop(0, count - 1, one, 0)

    @pl.when(count > 0)
    def _():
        with_units(backward_only, count - 1, jnp.maximum(count - 2, 0))


def gradient(counts, where, extended, amp, probe_modes, fwd, inv):
    modes, _, width, _ = probe_modes.shape
    vmem = pl.BlockSpec(memory_space=pltpu.VMEM)
    smem = pl.BlockSpec(memory_space=pltpu.SMEM)
    hbm = pl.BlockSpec(memory_space=pltpu.HBM)
    half = width // 2
    return pl.pallas_call(
        gradient_kernel,
        out_shape=jax.ShapeDtypeStruct(extended.shape, jnp.float32),
        in_specs=[smem, smem] + [vmem] * 3 + [hbm] * 2,
        out_specs=vmem,
        scratch_shapes=[
            pltpu.VMEM((2, width, width), jnp.float32),
            pltpu.VMEM((2, 2, width, width), jnp.bfloat16),
            pltpu.VMEM((modes, 2, width, width), jnp.float32),
            pltpu.VMEM((2, 2, width, width), jnp.bfloat16),
            pltpu.VMEM((2, width, width), jnp.float32),
            pltpu.VMEM((2, width, half), jnp.float32),
            pltpu.VMEM((2, width, half), jnp.float32),
            pltpu.VMEM(fwd.shape, jnp.bfloat16),
            pltpu.VMEM(inv.shape, jnp.bfloat16),
            pltpu.SemaphoreType.DMA((2,)),
        ],
        compiler_params=pltpu.CompilerParams(vmem_limit_bytes=40 * 1024 * 1024),
        name="gradient",
    )(counts, where, extended, amp, probe_modes, fwd, inv)


def exact(values, product):
    total = None
    for _ in range(3):
        piece = values.astype(jnp.bfloat16)
        values = values - piece.astype(jnp.float32)
        part = product(piece)
        total = part if total is None else total + part
    return total


def body(object_field, probe_modes, positions, counts, amplitude):
    width = probe_modes.shape[-1]
    fwd, inv = [pltpu.with_memory_space_constraint(x, pltpu.HBM) for x in tables(width)]
    where = positions[0, 0].T
    held = [pltpu.with_memory_space_constraint(x, pltpu.HBM) for x in (object_field, amplitude[0, 0])]
    extended, amp = exchange("spread", *held)
    for sweep in range(ITERS):
        total = gradient(counts, where, extended, amp, probe_modes, fwd, inv)
        (extended,) = exchange("both" if sweep < ITERS - 1 else "reduce", total, extended)
    return extended


def solution(mesh):
    placed = (
        P(None, "row", "col"),
        P(),
        P("row", "col", None, None),
        P("row", "col"),
        P("row", "col", None, None, None),
    )
    return jax.shard_map(
        body, mesh=mesh, in_specs=placed, out_specs=P(None, "row", "col"), check_vma=False
    )
```

```python
import functools
import math

import jax
import jax.numpy as jnp
import numpy as np
from jax import lax
from jax.experimental import pallas as pl
from jax.experimental.pallas import tpu as pltpu
from jax.sharding import PartitionSpec as P

ITERS = 2


step_size = 0.1
damping = 0.1


RIGHT_LOW, RIGHT_TOP, DOWN, UP, LEFT, LEFT_LOW = range(6)
UP_VIA, UP_ON, DOWN_VIA, DOWN_ON = range(6, 10)
SHARES = (9, 10, 8, 5)
PARTS = len(SHARES)


def exchange_kernel(mode, rows_of, cols_of, *refs):
    refs = list(refs)
    reduce, spread = mode != "spread", mode != "reduce"
    if reduce:
        tot_ref, ext_ref, out_ref = refs.pop(0), refs.pop(0), refs.pop(0)
        side_scr, top_scr, low_scr, above_scr = [refs.pop(0) for _ in range(4)]
        below_scr = refs.pop(0) if spread else None
        via_scr = refs.pop(0) if spread else None
        t = out_ref.shape[-1]
    else:
        field_ref, amp_ref = refs.pop(0), refs.pop(0)
        out_ref, sorted_ref, amp_scr, perm_scr, local_sem = [refs.pop(0) for _ in range(5)]
        t = field_ref.shape[-1]
    send_sem, recv_sem = refs
    unit = t // sum(SHARES)
    starts = [sum(SHARES[:i]) * unit for i in range(PARTS)]
    sizes = [share * unit for share in SHARES]
    r, c = lax.axis_index("row"), lax.axis_index("col")
    has_up, has_down = r > 0, r < rows_of - 1
    has_left, has_right = c > 0, c < cols_of - 1
    up = (jnp.where(has_up, r - 1, r + 1), c)
    down = (jnp.where(has_down, r + 1, r - 1), c)
    left = (r, jnp.where(has_left, c - 1, c + 1))
    right = (r, jnp.where(has_right, c + 1, c - 1))
    folded = reduce and spread and rows_of % 2 == 0 and rows_of > 2
    even, odd = lax.rem(r, 2) == 0, lax.rem(r, 2) == 1
    has_up2, has_down2 = r > 1, r < rows_of - 2
    up2 = (jnp.where(has_up2, r - 2, r + 2), c)
    down2 = (jnp.where(has_down2, r + 2, r - 2), c)
    far_up, far_down = jnp.logical_and(even, has_up), jnp.logical_and(odd, has_down)
    relay_up, relay_down = jnp.logical_and(even, has_down2), jnp.logical_and(odd, has_up2)

    def goes_round(i):
        return folded and i % 2 == 0

    def but(a, b):
        return jnp.logical_and(a, jnp.logical_not(b))

    if not reduce:
        own = pltpu.make_async_copy(field_ref, out_ref.at[0, :, pl.ds(0, t)], local_sem.at[0])
        own.start()
        measured = pltpu.make_async_copy(amp_ref, amp_scr, local_sem.at[1])
        measured.start()

    barrier = pltpu.get_barrier_semaphore()
    peers_of = [(has_up, up), (has_down, down), (has_left, left), (has_right, right)]
    if folded:
        peers_of += [(has_up2, up2), (has_down2, down2)]
    for there, device in peers_of:

        @pl.when(there)
        def _():
            pl.semaphore_signal(
                barrier, inc=1, device_id=device, device_id_type=pl.DeviceIdType.MESH
            )

    peers = sum(jnp.where(there, 1, 0) for there, _ in peers_of)
    pl.semaphore_wait(barrier, peers)

    def copy(kind, i):
        rows = pl.ds(starts[i], sizes[i])
        low = pl.ds(t + starts[i], sizes[i])
        if kind == RIGHT_LOW:
            src, dst, device = tot_ref.at[1, :, low], side_scr.at[:, low], right
        elif kind == RIGHT_TOP:
            src, dst, device = tot_ref.at[1, :, rows], side_scr.at[:, rows], right
        elif kind == DOWN:
            src, dst, device = low_scr.at[:, rows], above_scr.at[:, rows], down
        elif kind == UP and reduce:
            src, dst, device = top_scr.at[:, rows], below_scr.at[:, rows], up
        elif kind == UP:
            src, dst, device = field_ref.at[:, rows], out_ref.at[0, :, low], up
        elif kind == UP_VIA:
            src, dst, device = top_scr.at[:, rows], via_scr.at[:, rows], up2
        elif kind == UP_ON:
            src, dst, device = via_scr.at[:, rows], below_scr.at[:, rows], down
        elif kind == DOWN_VIA:
            src, dst, device = low_scr.at[:, rows], via_scr.at[:, rows], down2
        elif kind == DOWN_ON:
            src, dst, device = via_scr.at[:, rows], above_scr.at[:, rows], up
        elif kind == LEFT and reduce:
            src, dst, device = out_ref.at[0, :, rows], out_ref.at[1, :, rows], left
        elif kind == LEFT:
            src, dst, device = field_ref.at[:, rows], out_ref.at[1, :, rows], left
        else:
            src, dst, device = out_ref.at[0, :, low], out_ref.at[1, :, low], left
        return pltpu.make_async_remote_copy(
            src_ref=src,
            dst_ref=dst,
            send_sem=send_sem.at[kind, i],
            recv_sem=recv_sem.at[kind, i],
            device_id=device,
            device_id_type=pl.DeviceIdType.MESH,
        )

    def start(there, kind, i):
        @pl.when(there)
        def _():
            copy(kind, i).start()

    def got(there, kind, i):
        @pl.when(there)
        def _():
            copy(kind, i).wait_recv()

    def sent(there, kind, parts=range(PARTS)):
        @pl.when(there)
        def _():
            for i in parts:
                copy(kind, i).wait_send()

    if reduce:
        for i in range(PARTS):
            start(jnp.logical_and(has_right, even) if spread else has_right, RIGHT_LOW, i)
            if spread:
                start(has_right, RIGHT_TOP, i)
                start(jnp.logical_and(has_right, odd), RIGHT_LOW, i)
        if not spread:
            for i in range(PARTS):
                start(has_right, RIGHT_TOP, i)

        @pl.when(jnp.logical_not(has_left))
        def _():
            side_scr[...] = jnp.zeros_like(side_scr)

        @pl.when(jnp.logical_not(has_up))
        def _():
            above_scr[...] = jnp.zeros_like(above_scr)

    if spread:

        @pl.when(jnp.logical_not(has_down))
        def _():
            out_ref[0, :, t:] = jnp.zeros((2, t, t), jnp.float32)

        @pl.when(jnp.logical_not(has_right))
        def _():
            out_ref[1] = jnp.zeros((2, 2 * t, t), jnp.float32)

        @pl.when(jnp.logical_and(has_right, jnp.logical_not(has_down)))
        def _():
            out_ref[1, :, t:] = jnp.zeros((2, t, t), jnp.float32)

    def band(i):
        first, end = starts[i], starts[i] + sizes[i]
        return slice(first, end), slice(t + first, t + end)

    both = jnp.logical_and(has_down, has_left)
    if reduce:
        def ready(i):
            rows, low = band(i)
            got(has_left, RIGHT_LOW, i)

            @pl.when(has_down)
            def _():
                low_scr[:, rows] = tot_ref[0, :, low] + side_scr[:, low]

            if spread:
                got(has_left, RIGHT_TOP, i)
                top_scr[:, rows] = tot_ref[0, :, rows] + side_scr[:, rows]

        def within(i):
            start(jnp.logical_and(odd, has_up), UP, i)
            start(jnp.logical_and(even, has_down), DOWN, i)

        def across(i):
            start(far_up, UP_VIA if goes_round(i) else UP, i)
            start(far_down, DOWN_VIA if goes_round(i) else DOWN, i)

        def pass_on(i):
            got(relay_up, UP_VIA, i)
            start(relay_up, UP_ON, i)
            got(relay_down, DOWN_VIA, i)
            start(relay_down, DOWN_ON, i)

        def own_band(there, i, kinds):
            rows, _ = band(i)

            @pl.when(there)
            def _():
                for also, kind in kinds:
                    got(also, kind, i)
                out_ref[0, :, rows] = ext_ref[0, :, rows] - step_size * (
                    top_scr[:, rows] + above_scr[:, rows]
                )
                start(has_left, LEFT, i)

        def low_band(there, i, kinds):
            rows, low = band(i)

            @pl.when(jnp.logical_and(there, has_down))
            def _():
                for also, kind in kinds:
                    got(also, kind, i)
                out_ref[0, :, low] = ext_ref[0, :, low] - step_size * (
                    low_scr[:, rows] + below_scr[:, rows]
                )
                start(has_left, LEFT_LOW, i)

        def settle_within(i):
            low_band(even, i, [(has_down, UP)])
            own_band(odd, i, [(has_up, DOWN)])

        def settle_across(i):
            own_band(even, i, [(has_up, DOWN_ON if goes_round(i) else DOWN)])
            low_band(odd, i, [(has_down, UP_ON if goes_round(i) else UP)])

        if spread and folded:
            for i in range(0, PARTS, 2):
                ready(i)
                if i > 0:
                    pass_on(i - 2)
                within(i)
                across(i)
                ready(i + 1)
                if i == 0:
                    within(i + 1)
                    across(i + 1)
                else:
                    across(i + 1)
                    within(i + 1)
            late = PARTS - 2
            settle_within(0)
            settle_within(1)
            pass_on(late)
            for i in range(PARTS):
                settle_across(i)
                if i > 0 and i + 1 < PARTS:
                    settle_within(i + 1)
        elif spread:
            for i in range(PARTS):
                ready(i)
                within(i)
                across(i)
            for i in range(PARTS):
                settle_within(i)
                settle_across(i)
        for i in range(PARTS):
            rows, low = band(i)
            if spread:
                continue
            ready(i)
            start(has_down, DOWN, i)
        for i in range(PARTS):
            rows, low = band(i)
            if spread:
                continue
            got(has_left, RIGHT_TOP, i)
            got(has_up, DOWN, i)
            out_ref[:, rows] = ext_ref[0, :, rows] - step_size * (
                (tot_ref[0, :, rows] + side_scr[:, rows]) + above_scr[:, rows]
            )
    else:
        for i in range(PARTS):
            start(has_up, UP, i)
            start(has_left, LEFT, i)
        spot = lax.broadcasted_iota(jnp.int32, (t, t), 1)
        spot = jnp.where(spot < t // 2, 2 * spot, 2 * spot - (t - 1))
        perm = jnp.where(lax.broadcasted_iota(jnp.int32, (t, t), 0) == spot, 1.0, 0.0)
        perm_scr[0] = perm.astype(jnp.bfloat16)
        spot = lax.broadcasted_iota(jnp.int32, (t, t), 0)
        spot = jnp.where(spot < t // 2, 2 * spot, 2 * spot - (t - 1))
        perm = jnp.where(lax.broadcasted_iota(jnp.int32, (t, t), 1) == spot, 1.0, 0.0)
        perm_scr[1] = perm.astype(jnp.bfloat16)
        measured.wait()
        slots = amp_ref.shape[0]
        done = 0
        for i in range(PARTS):
            until = min(slots, -(-slots * (i + 1) // (PARTS - 2)))

            def one(s, carry):
                cols = exact(amp_scr[s], lambda piece: dot(piece, perm_scr[0]))
                sorted_ref[s] = exact(cols, lambda piece: dot(perm_scr[1], piece))
                return carry

            lax.fori_loop(done, until, one, 0)
            done = until
            got(has_down, UP, i)
            start(both, LEFT_LOW, i)
    if not reduce:
        own.wait()
    if spread:
        for i in range(PARTS):
            got(has_right, LEFT, i)
            got(jnp.logical_and(has_right, has_down), LEFT_LOW, i)
    round_parts = [i for i in range(PARTS) if goes_round(i)]
    plain_parts = [i for i in range(PARTS) if not goes_round(i)]
    if reduce:
        sent(has_right, RIGHT_LOW)
        sent(has_right, RIGHT_TOP)
        sent(has_down, DOWN, plain_parts)
    if folded:
        sent(but(has_down, far_down), DOWN, round_parts)
        sent(far_down, DOWN_VIA, round_parts)
        sent(relay_down, DOWN_ON, round_parts)
        sent(but(has_up, far_up), UP, round_parts)
        sent(far_up, UP_VIA, round_parts)
        sent(relay_up, UP_ON, round_parts)
    if spread:
        sent(has_up, UP, plain_parts)
        sent(has_left, LEFT)
        sent(both, LEFT_LOW)


def exchange(mode, *operands):
    planes, t = operands[0].shape[-3], operands[0].shape[-1]
    vmem = pl.BlockSpec(memory_space=pltpu.VMEM)
    tile = jax.ShapeDtypeStruct((planes, t, t), jnp.float32)
    shapes = [tile if mode == "reduce" else jax.ShapeDtypeStruct((2, planes, 2 * t, t), jnp.float32)]
    specs = [vmem] * len(operands)
    if mode == "spread":
        amp = operands[1]
        specs = [pl.BlockSpec(memory_space=pltpu.HBM)] * 2
        shapes.append(jax.ShapeDtypeStruct(amp.shape, jnp.float32))
        scratch = [
            pltpu.VMEM(amp.shape, jnp.float32),
            pltpu.VMEM((2, t, t), jnp.bfloat16),
            pltpu.SemaphoreType.DMA((2,)),
        ]
    else:
        scratch = [pltpu.VMEM((planes, 2 * t, t), jnp.float32)]
        scratch += [pltpu.VMEM((planes, t, t), jnp.float32)] * (5 if mode == "both" else 3)
    scratch += [pltpu.SemaphoreType.DMA((10, PARTS))] * 2
    kernel = functools.partial(
        exchange_kernel, mode, lax.axis_size("row"), lax.axis_size("col")
    )
    return pl.pallas_call(
        kernel,
        out_shape=shapes,
        in_specs=specs,
        out_specs=[vmem] * len(shapes),
        scratch_shapes=scratch,
        compiler_params=pltpu.CompilerParams(
            collective_id=("spread", "both", "reduce").index(mode),
            has_side_effects=True,
            vmem_limit_bytes=24 * 1024 * 1024,
        ),
        name="exchange_" + mode,
    )(*operands)


def tables(width):
    half = width // 2
    ladder = np.arange(width)
    theta = (ladder[:, None] * ladder[None, :] % width) * (2.0 * math.pi / width)
    factor = 1.0 / math.sqrt(width)
    cosine = np.cos(theta) * factor
    sine = np.sin(theta) * factor
    out = []
    for parity in (0, 1):
        c = cosine[parity::2, :half]
        s = sine[parity::2, :half]
        out.append(np.block([[c, s], [-s, c]]))
    stacked = np.stack(out).astype(np.float32)
    fwd = jnp.asarray(stacked).astype(jnp.bfloat16)
    inv = jnp.asarray(np.ascontiguousarray(stacked.transpose(0, 2, 1))).astype(jnp.bfloat16)
    return fwd, inv


def dot(a, b):
    return jnp.dot(a, b, preferred_element_type=jnp.float32)


ROWS_OF_CHUNK = 16


def interleave(first, second):
    out, total = [], len(first) + len(second)
    i = j = 0
    for _ in range(total):
        if j >= len(second) or (i < len(first) and i * len(second) <= j * len(first)):
            out.append(first[i])
            i += 1
        else:
            out.append(second[j])
            j += 1
    return out


class Chunks:
    def __init__(self, refs):
        self.free = [list(refs[0]), list(refs[1])]
        self.held = {}

    def feed(self, unit, key, lhs, staged=None):
        ref = self.free[unit].pop(0)
        self.held[unit, key] = ref
        pltpu.matmul_acc_lhs(ref, lhs, load_staged_rhs=staged)

    def pop(self, unit, key):
        ref = self.held.pop((unit, key))
        self.free[unit].append(ref)
        return pltpu.matmul_pop(ref)


class Step:
    def __init__(self, refs, acc):
        self.__dict__.update(refs)
        self.acc = acc
        self.modes, _, self.width, _ = self.probe.shape
        self.h = self.width // 2
        self.flip = 0

    def corner(self, s):
        lane, sub = 128, 8
        top, left = self.pos[0, s], self.pos[1, s]
        base = left // lane
        rest = left - base * lane
        over = pl.multiple_of((top // sub) * sub, sub)
        return base, rest, over, top - over

    def block_of(self, base, c):
        lane = 128
        per = self.width // lane
        half = (base + c) // per
        near = base + c - half * per
        return half, pl.ds(pl.multiple_of(near * lane, lane), lane)

    def cut_patch(self, s):
        lane, sub, width = 128, 8, self.width
        base, rest, over, drop = self.corner(s)
        part = 64
        units = []
        lanes = lax.broadcasted_iota(jnp.int32, (part, lane), 1)
        ledge = lax.broadcasted_iota(jnp.int32, (part // sub, sub, lane), 1)

        def unit(d, r):
            turned = []
            for c in range(width // lane + 1):
                half, cols = self.block_of(base, c)
                rows = pl.ds(pl.multiple_of(over + r, sub), part + sub)
                x = self.ext[half, d, rows, cols].reshape(part // sub + 1, sub, lane)
                x = pltpu.roll(x, lax.rem(sub - drop, sub), 1)
                x = jnp.where(ledge + drop < sub, x[:-1], x[1:]).reshape(part, lane)
                turned.append(pltpu.roll(x, lax.rem(lane - rest, lane), 1))
            for c in range(width // lane):
                self.patch[d, r : r + part, c * lane : (c + 1) * lane] = jnp.where(
                    lanes + rest < lane, turned[c], turned[c + 1]
                )

        for r in range(0, width, part):
            for d in range(2):
                units.append(functools.partial(unit, d, r))
        return units

    def make_psi(self, m):
        h, step = self.h, 16
        out = self.psi.at[m % 2]

        def unit(r):
            rows, low = slice(r, r + step), slice(h + r, h + r + step)
            pr, pi = self.probe[m, 0, rows], self.probe[m, 1, rows]
            qr, qi = self.probe[m, 0, low], self.probe[m, 1, low]
            fr, fi = self.patch[0, rows], self.patch[1, rows]
            gr, gi = self.patch[0, low], self.patch[1, low]
            ur, ui = pr * fr - pi * fi, pr * fi + pi * fr
            vr, vi = qr * gr - qi * gi, qr * gi + qi * gr
            out[0, rows] = (ur + vr).astype(jnp.bfloat16)
            out[0, low] = (ui + vi).astype(jnp.bfloat16)
            out[1, rows] = (ur - vr).astype(jnp.bfloat16)
            out[1, low] = (ui - vi).astype(jnp.bfloat16)

        return [functools.partial(unit, r) for r in range(0, h, step)]

    def weigh(self, m, s):
        n, h = ROWS_OF_CHUNK, self.h

        def unit(q, r):
            rows = slice(r, r + n)
            far = self.acc.pop(q, ("R1", m, r))
            self.far[m, q, rows] = far
            re, im = far[:, :h], far[:, h:]
            term = re * re + im * im
            if m > 0:
                term = self.bright[q, rows] + term
            if m < self.modes - 1:
                self.bright[q, rows] = term
            else:
                seen = self.amp[s, rows, q * h : (q + 1) * h]
                self.ratio[q, rows] = 1.0 - seen * lax.rsqrt(term + damping)

        return [functools.partial(unit, q, r) for r in range(0, self.width, n) for q in range(2)]

    def make_chi(self, m):
        n, h = ROWS_OF_CHUNK, self.h
        out = self.chi.at[m % 2]

        def unit(p, r):
            for q in range(2):
                cols = slice(q * h, (q + 1) * h)
                rows = slice(p * h + r, p * h + r + n)
                ratio = self.ratio[q, rows]
                out[p, r : r + n, cols] = (self.far[m, q, rows, :h] * ratio).astype(jnp.bfloat16)
                out[p, h + r : h + r + n, cols] = (self.far[m, q, rows, h:] * ratio).astype(
                    jnp.bfloat16
                )

        return [functools.partial(unit, p, r) for r in range(0, h, n) for p in range(2)]

    def gather(self, m):
        n, h = ROWS_OF_CHUNK, self.h

        def unit(r):
            rows = slice(r, r + n)
            even, odd = self.acc.pop(0, ("R2", m, r)), self.acc.pop(1, ("R2", m, r))
            for cols, wave in ((slice(0, h), even + odd), (slice(h, 2 * h), even - odd)):
                wr, wi = wave[:, :h], wave[:, h:]
                pr, pi = self.probe[m, 0, rows, cols], self.probe[m, 1, rows, cols]
                gr, gi = pr * wr + pi * wi, pr * wi - pi * wr
                if m > 0:
                    gr, gi = self.grad[0, rows, cols] + gr, self.grad[1, rows, cols] + gi
                self.grad[0, rows, cols] = gr
                self.grad[1, rows, cols] = gi

        return [functools.partial(unit, r) for r in range(0, self.width, n)]

    def place(self, s):
        lane, sub, width = 128, 8, self.width
        base, rest, over, drop = self.corner(s)
        wide = width // lane + 1
        blocks = width // sub
        part = 64
        lanes = lax.broadcasted_iota(jnp.int32, (part, lane), 1)

        def unit(d, r):
            edge = jnp.zeros((part, lane), jnp.float32)
            turned = [edge]
            for c in range(width // lane):
                x = self.grad[d, r : r + part, c * lane : (c + 1) * lane]
                turned.append(pltpu.roll(x, rest, 1))
            turned.append(edge)
            for c in range(wide):
                x = jnp.where(lanes >= rest, turned[c + 1], turned[c])
                x = pltpu.roll(x.reshape(part // sub, sub, lane), drop, 1)
                brim = jnp.zeros((1, sub, lane), jnp.float32)
                after = jnp.concatenate([x, brim], axis=0)
                before = jnp.concatenate([brim, x], axis=0)
                rim = lax.broadcasted_iota(jnp.int32, (part // sub + 1, sub, lane), 1)
                x = jnp.where(rim >= drop, after, before).reshape(part + sub, lane)
                half, cols = self.block_of(base, c)
                spot = (half, d, pl.ds(pl.multiple_of(over + r, sub), part + sub), cols)
                self.tot[spot] = self.tot[spot] + x

        return [functools.partial(unit, d, r) for r in range(0, width, part) for d in range(2)]

    def left(self, kind, m):
        n, h = ROWS_OF_CHUNK, self.h
        rhs, lhs = (self.psi, self.a) if kind == "L1" else (self.chi, self.b)
        reg = self.flip
        self.flip = 1 - reg

        def push():
            for unit in range(2):
                pltpu.matmul_push_rhs(rhs[m % 2, unit], reg, unit)

        def feed(r, first):
            for unit in range(2):
                self.acc.feed(unit, (kind, m, r), lhs[unit, r : r + n], reg if first else None)

        order = [r + d for r in range(0, h, n) for d in (0, h)]
        return push, [functools.partial(feed, r, k == 0) for k, r in enumerate(order)]

    def right(self, kind, m):
        n, h = ROWS_OF_CHUNK, self.h
        rhs = self.b if kind == "R1" else self.a
        reg = self.flip
        self.flip = 1 - reg

        def push():
            for unit in range(2):
                pltpu.matmul_push_rhs(rhs[unit], reg, unit)

        def feed_forward(r, p, first):
            re, im = self.acc.pop(p, ("L1", m, r)), self.acc.pop(p, ("L1", m, h + r))
            re_l, re_r, im_l, im_r = re[:, :h], re[:, h:], im[:, :h], im[:, h:]
            plus = jnp.concatenate([re_l + re_r, im_l + im_r], axis=1).astype(jnp.bfloat16)
            less = jnp.concatenate([re_l - re_r, im_l - im_r], axis=1).astype(jnp.bfloat16)
            for unit, x in enumerate((plus, less)):
                self.acc.feed(unit, (kind, m, p * h + r), x, reg if first else None)

        def feed_backward(r, first):
            key = ("L2", m, r), ("L2", m, h + r)
            ere, oim = self.acc.pop(0, key[0]), self.acc.pop(1, key[1])
            ore, eim = self.acc.pop(1, key[0]), self.acc.pop(0, key[1])
            for k, (re, im) in enumerate(((ere + ore, eim + oim), (ere - ore, eim - oim))):
                for unit in range(2):
                    cols = slice(unit * h, (unit + 1) * h)
                    y = jnp.concatenate([re[:, cols], im[:, cols]], axis=1).astype(jnp.bfloat16)
                    self.acc.feed(
                        unit, (kind, m, k * h + r), y, reg if first and k == 0 else None
                    )

        if kind == "R1":
            spots = [(r, p) for r in range(0, h, n) for p in range(2)]
            feeds = [functools.partial(feed_forward, r, p, k == 0) for k, (r, p) in enumerate(spots)]
        else:
            feeds = [functools.partial(feed_backward, r, r == 0) for r in range(0, h, n)]
        return push, feeds

    def run(self, jobs):
        built = []
        for kind, m, beside in jobs:
            if kind is None:
                built.append((None, [], beside))
                continue
            push, feeds = (self.left if kind[0] == "L" else self.right)(kind, m)
            built.append((push, feeds, beside))
        for k, (push, feeds, beside) in enumerate(built):
            if push is not None and (k == 0 or built[k - 1][0] is None):
                push()
            for unit in interleave(beside, feeds):
                unit()
            if push is not None and k + 1 < len(built) and built[k + 1][0] is not None:
                built[k + 1][0]()


def forward_only(step, s, ahead, ready, blank):
    psi, weigh = step.make_psi, lambda m: step.weigh(m, s)
    for unit in step.cut_patch(s) + psi(0):
        unit()
    ready()
    step.run(
        [
            ("L1", 0, psi(1)),
            ("L1", 1, psi(2)),
            ("R1", 0, psi(3)),
            ("L1", 2, weigh(0)),
            ("R1", 1, step.cut_patch(ahead)),
            ("L1", 3, weigh(1) + blank[:16]),
            ("R1", 2, psi(0) + blank[16:]),
            ("R1", 3, weigh(2)),
            (None, 0, weigh(3)),
        ]
    )


def backward_only(step, s, behind):
    chi, gather, place = step.make_chi, step.gather, step.place(behind)
    half = len(place) // 2
    step.run(
        [
            (None, 0, chi(0)),
            ("L2", 0, chi(1) + place[:half]),
            ("L2", 1, chi(2) + place[half:]),
            ("R2", 0, []),
            ("L2", 2, chi(3) + gather(0)),
            ("R2", 1, []),
            ("L2", 3, gather(1)),
            ("R2", 2, []),
            ("R2", 3, gather(2)),
            (None, 0, gather(3) + step.place(s)),
        ]
    )


def both_ways(step, behind, back, ahead, beyond):
    psi, weigh = step.make_psi, lambda m: step.weigh(m, ahead)
    chi, gather = step.make_chi, step.gather
    cut, place = step.cut_patch(beyond), step.place(behind)
    psi1, psi2, psi3, psi0 = psi(1), psi(2), psi(3), psi(0)
    step.run(
        [
            ("L1", 0, interleave(chi(0), psi1[:3])),
            ("L2", 0, interleave(chi(1), psi1[3:])),
            ("L1", 1, place[:5]),
            ("R2", 0, place[5:]),
            ("L2", 1, psi2),
            ("R1", 0, gather(0)),
            ("R2", 1, chi(2)),
            ("L2", 2, interleave(chi(3), weigh(0))),
            ("L1", 2, psi3),
            ("R2", 2, gather(1)),
            ("L2", 3, cut),
            ("R1", 1, gather(2)),
            ("L1", 3, weigh(1)),
            ("R2", 3, psi0),
            ("R1", 2, []),
            ("R1", 3, interleave(gather(3), weigh(2))),
            (None, 0, weigh(3)),
        ]
    )


NAMES = ("count", "pos", "ext", "amp", "probe", "a_hbm", "b_hbm", "tot")
NAMES += ("patch", "psi", "far", "chi", "grad", "bright", "ratio", "a", "b", "sem")


def gradient_kernel(*operands):
    refs = dict(zip(NAMES, operands))
    sem = refs["sem"]
    fetch = [
        pltpu.make_async_copy(refs[name + "_hbm"], refs[name], sem.at[k])
        for k, name in enumerate("ab")
    ]
    for copy in fetch:
        copy.start()
    tot = refs["tot"]

    def clear(half, d, r):
        part = 64
        tot[half, d, r : r + part] = jnp.zeros((part, tot.shape[3]), jnp.float32)

    blank = [
        functools.partial(clear, half, d, r)
        for half in range(2)
        for d in range(2)
        for r in range(0, tot.shape[2], 64)
    ]
    refs["grad"][...] = jnp.zeros_like(refs["grad"])
    count = refs["count"][0, 0]
    last = refs["amp"].shape[0] - 1

    def with_units(work, *where):
        def body(*acc):
            half = len(acc) // 2
            work(Step(refs, Chunks((acc[:half], acc[half:]))), *where)

        depth = 1024 // ROWS_OF_CHUNK
        shape = (ROWS_OF_CHUNK, refs["probe"].shape[-1])
        pl.run_scoped(body, *[pltpu.ACC(u)(shape, jnp.float32) for u in (0, 1) for _ in range(depth)])

    def ready():
        for copy in fetch:
            copy.wait()

    @pl.when(count > 0)
    def _():
        with_units(forward_only, 0, min(1, last), ready, blank)

    @pl.when(count <= 0)
    def _():
        for unit in blank:
            unit()
        ready()

    def one(s, carry):
        with_units(both_ways, jnp.maximum(s - 1, 0), s, s + 1, jnp.minimum(s + 2, last))
        return carry

    lax.fori_loop(0, count - 1, one, 0)

    @pl.when(count > 0)
    def _():
        with_units(backward_only, count - 1, jnp.maximum(count - 2, 0))


def gradient(counts, where, extended, amp, probe_modes, fwd, inv):
    modes, _, width, _ = probe_modes.shape
    vmem = pl.BlockSpec(memory_space=pltpu.VMEM)
    smem = pl.BlockSpec(memory_space=pltpu.SMEM)
    hbm = pl.BlockSpec(memory_space=pltpu.HBM)
    half = width // 2
    return pl.pallas_call(
        gradient_kernel,
        out_shape=jax.ShapeDtypeStruct(extended.shape, jnp.float32),
        in_specs=[smem, smem] + [vmem] * 3 + [hbm] * 2,
        out_specs=vmem,
        scratch_shapes=[
            pltpu.VMEM((2, width, width), jnp.float32),
            pltpu.VMEM((2, 2, width, width), jnp.bfloat16),
            pltpu.VMEM((modes, 2, width, width), jnp.float32),
            pltpu.VMEM((2, 2, width, width), jnp.bfloat16),
            pltpu.VMEM((2, width, width), jnp.float32),
            pltpu.VMEM((2, width, half), jnp.float32),
            pltpu.VMEM((2, width, half), jnp.float32),
            pltpu.VMEM(fwd.shape, jnp.bfloat16),
            pltpu.VMEM(inv.shape, jnp.bfloat16),
            pltpu.SemaphoreType.DMA((2,)),
        ],
        compiler_params=pltpu.CompilerParams(vmem_limit_bytes=40 * 1024 * 1024),
        name="gradient",
    )(counts, where, extended, amp, probe_modes, fwd, inv)


def exact(values, product):
    total = None
    for _ in range(3):
        piece = values.astype(jnp.bfloat16)
        values = values - piece.astype(jnp.float32)
        part = product(piece)
        total = part if total is None else total + part
    return total


def body(object_field, probe_modes, positions, counts, amplitude):
    width = probe_modes.shape[-1]
    fwd, inv = [pltpu.with_memory_space_constraint(x, pltpu.HBM) for x in tables(width)]
    where = positions[0, 0].T
    held = [pltpu.with_memory_space_constraint(x, pltpu.HBM) for x in (object_field, amplitude[0, 0])]
    extended, amp = exchange("spread", *held)
    for sweep in range(ITERS):
        total = gradient(counts, where, extended, amp, probe_modes, fwd, inv)
        (extended,) = exchange("both" if sweep < ITERS - 1 else "reduce", total, extended)
    return extended


def solution(mesh):
    placed = (
        P(None, "row", "col"),
        P(),
        P("row", "col", None, None),
        P("row", "col"),
        P("row", "col", None, None, None),
    )
    return jax.shard_map(
        body, mesh=mesh, in_specs=placed, out_specs=P(None, "row", "col"), check_vma=False
    )
```

```python
import functools
import math

import jax
import jax.numpy as jnp
import numpy as np
from jax import lax
from jax.experimental import pallas as pl
from jax.experimental.pallas import tpu as pltpu
from jax.sharding import PartitionSpec as P

ITERS = 2


step_size = 0.1
damping = 0.1


RIGHT_LOW, RIGHT_TOP, DOWN, UP, LEFT, LEFT_LOW = range(6)
UP_VIA, UP_ON, DOWN_VIA, DOWN_ON = range(6, 10)
SHARES = (9, 10, 8, 5)
PARTS = len(SHARES)


def exchange_kernel(mode, rows_of, cols_of, *refs):
    refs = list(refs)
    reduce, spread = mode != "spread", mode != "reduce"
    if reduce:
        tot_ref, ext_ref, out_ref = refs.pop(0), refs.pop(0), refs.pop(0)
        side_scr, top_scr, low_scr, above_scr = [refs.pop(0) for _ in range(4)]
        below_scr = refs.pop(0) if spread else None
        via_scr = refs.pop(0) if spread else None
        t = out_ref.shape[-1]
    else:
        field_ref, amp_ref, *table_refs = [refs.pop(0) for _ in range(4)]
        out_ref, sorted_ref, *held_refs = [refs.pop(0) for _ in range(4)]
        amp_scr, perm_scr, local_sem = [refs.pop(0) for _ in range(3)]
        t = field_ref.shape[-1]
    send_sem, recv_sem = refs
    unit = t // sum(SHARES)
    starts = [sum(SHARES[:i]) * unit for i in range(PARTS)]
    sizes = [share * unit for share in SHARES]
    r, c = lax.axis_index("row"), lax.axis_index("col")
    has_up, has_down = r > 0, r < rows_of - 1
    has_left, has_right = c > 0, c < cols_of - 1
    up = (jnp.where(has_up, r - 1, r + 1), c)
    down = (jnp.where(has_down, r + 1, r - 1), c)
    left = (r, jnp.where(has_left, c - 1, c + 1))
    right = (r, jnp.where(has_right, c + 1, c - 1))
    folded = reduce and spread and rows_of % 2 == 0 and rows_of > 2
    even, odd = lax.rem(r, 2) == 0, lax.rem(r, 2) == 1
    has_up2, has_down2 = r > 1, r < rows_of - 2
    up2 = (jnp.where(has_up2, r - 2, r + 2), c)
    down2 = (jnp.where(has_down2, r + 2, r - 2), c)
    far_up, far_down = jnp.logical_and(even, has_up), jnp.logical_and(odd, has_down)
    relay_up, relay_down = jnp.logical_and(even, has_down2), jnp.logical_and(odd, has_up2)

    def goes_round(i):
        return folded and i % 2 == 0

    def but(a, b):
        return jnp.logical_and(a, jnp.logical_not(b))

    if not reduce:
        own = pltpu.make_async_copy(field_ref, out_ref.at[0, :, pl.ds(0, t)], local_sem.at[0])
        own.start()
        measured = pltpu.make_async_copy(amp_ref, amp_scr, local_sem.at[1])
        measured.start()
        holds = [
            pltpu.make_async_copy(table_refs[k], held_refs[k], local_sem.at[2 + k]) for k in range(2)
        ]
        for hold in holds:
            hold.start()

    barrier = pltpu.get_barrier_semaphore()
    peers_of = [(has_up, up), (has_down, down), (has_left, left), (has_right, right)]
    if folded:
        peers_of += [(has_up2, up2), (has_down2, down2)]
    for there, device in peers_of:

        @pl.when(there)
        def _():
            pl.semaphore_signal(
                barrier, inc=1, device_id=device, device_id_type=pl.DeviceIdType.MESH
            )

    peers = sum(jnp.where(there, 1, 0) for there, _ in peers_of)
    pl.semaphore_wait(barrier, peers)

    def copy(kind, i):
        rows = pl.ds(starts[i], sizes[i])
        low = pl.ds(t + starts[i], sizes[i])
        if kind == RIGHT_LOW:
            src, dst, device = tot_ref.at[1, :, low], side_scr.at[:, low], right
        elif kind == RIGHT_TOP:
            src, dst, device = tot_ref.at[1, :, rows], side_scr.at[:, rows], right
        elif kind == DOWN:
            src, dst, device = low_scr.at[:, rows], above_scr.at[:, rows], down
        elif kind == UP and reduce:
            src, dst, device = top_scr.at[:, rows], below_scr.at[:, rows], up
        elif kind == UP:
            src, dst, device = field_ref.at[:, rows], out_ref.at[0, :, low], up
        elif kind == UP_VIA:
            src, dst, device = top_scr.at[:, rows], via_scr.at[:, rows], up2
        elif kind == UP_ON:
            src, dst, device = via_scr.at[:, rows], below_scr.at[:, rows], down
        elif kind == DOWN_VIA:
            src, dst, device = low_scr.at[:, rows], via_scr.at[:, rows], down2
        elif kind == DOWN_ON:
            src, dst, device = via_scr.at[:, rows], above_scr.at[:, rows], up
        elif kind == LEFT and reduce:
            src, dst, device = out_ref.at[0, :, rows], out_ref.at[1, :, rows], left
        elif kind == LEFT:
            src, dst, device = field_ref.at[:, rows], out_ref.at[1, :, rows], left
        else:
            src, dst, device = out_ref.at[0, :, low], out_ref.at[1, :, low], left
        return pltpu.make_async_remote_copy(
            src_ref=src,
            dst_ref=dst,
            send_sem=send_sem.at[kind, i],
            recv_sem=recv_sem.at[kind, i],
            device_id=device,
            device_id_type=pl.DeviceIdType.MESH,
        )

    def start(there, kind, i):
        @pl.when(there)
        def _():
            copy(kind, i).start()

    def got(there, kind, i):
        @pl.when(there)
        def _():
            copy(kind, i).wait_recv()

    def sent(there, kind, parts=range(PARTS)):
        @pl.when(there)
        def _():
            for i in parts:
                copy(kind, i).wait_send()

    if reduce:
        for i in range(PARTS):
            start(jnp.logical_and(has_right, even) if spread else has_right, RIGHT_LOW, i)
            if spread:
                start(has_right, RIGHT_TOP, i)
                start(jnp.logical_and(has_right, odd), RIGHT_LOW, i)
        if not spread:
            for i in range(PARTS):
                start(has_right, RIGHT_TOP, i)

        @pl.when(jnp.logical_not(has_left))
        def _():
            side_scr[...] = jnp.zeros_like(side_scr)

        @pl.when(jnp.logical_not(has_up))
        def _():
            above_scr[...] = jnp.zeros_like(above_scr)

    if spread:

        @pl.when(jnp.logical_not(has_down))
        def _():
            out_ref[0, :, t:] = jnp.zeros((2, t, t), jnp.float32)

        @pl.when(jnp.logical_not(has_right))
        def _():
            out_ref[1] = jnp.zeros((2, 2 * t, t), jnp.float32)

        @pl.when(jnp.logical_and(has_right, jnp.logical_not(has_down)))
        def _():
            out_ref[1, :, t:] = jnp.zeros((2, t, t), jnp.float32)

    def band(i):
        first, end = starts[i], starts[i] + sizes[i]
        return slice(first, end), slice(t + first, t + end)

    both = jnp.logical_and(has_down, has_left)
    if reduce:
        def ready(i):
            rows, low = band(i)
            got(has_left, RIGHT_LOW, i)

            @pl.when(has_down)
            def _():
                low_scr[:, rows] = tot_ref[0, :, low] + side_scr[:, low]

            if spread:
                got(has_left, RIGHT_TOP, i)
                top_scr[:, rows] = tot_ref[0, :, rows] + side_scr[:, rows]

        def within(i):
            start(jnp.logical_and(odd, has_up), UP, i)
            start(jnp.logical_and(even, has_down), DOWN, i)

        def across(i):
            start(far_up, UP_VIA if goes_round(i) else UP, i)
            start(far_down, DOWN_VIA if goes_round(i) else DOWN, i)

        def pass_on(i):
            got(relay_up, UP_VIA, i)
            start(relay_up, UP_ON, i)
            got(relay_down, DOWN_VIA, i)
            start(relay_down, DOWN_ON, i)

        def own_band(there, i, kinds):
            rows, _ = band(i)

            @pl.when(there)
            def _():
                for also, kind in kinds:
                    got(also, kind, i)
                out_ref[0, :, rows] = ext_ref[0, :, rows] - step_size * (
                    top_scr[:, rows] + above_scr[:, rows]
                )
                start(has_left, LEFT, i)

        def low_band(there, i, kinds):
            rows, low = band(i)

            @pl.when(jnp.logical_and(there, has_down))
            def _():
                for also, kind in kinds:
                    got(also, kind, i)
                out_ref[0, :, low] = ext_ref[0, :, low] - step_size * (
                    low_scr[:, rows] + below_scr[:, rows]
                )
                start(has_left, LEFT_LOW, i)

        def settle_within(i):
            low_band(even, i, [(has_down, UP)])
            own_band(odd, i, [(has_up, DOWN)])

        def settle_across(i):
            own_band(even, i, [(has_up, DOWN_ON if goes_round(i) else DOWN)])
            low_band(odd, i, [(has_down, UP_ON if goes_round(i) else UP)])

        if spread and folded:
            for i in range(0, PARTS, 2):
                ready(i)
                if i > 0:
                    pass_on(i - 2)
                within(i)
                across(i)
                ready(i + 1)
                if i == 0:
                    within(i + 1)
                    across(i + 1)
                else:
                    across(i + 1)
                    within(i + 1)
            late = PARTS - 2
            settle_within(0)
            settle_within(1)
            pass_on(late)
            for i in range(PARTS):
                settle_across(i)
                if i > 0 and i + 1 < PARTS:
                    settle_within(i + 1)
        elif spread:
            for i in range(PARTS):
                ready(i)
                within(i)
                across(i)
            for i in range(PARTS):
                settle_within(i)
                settle_across(i)
        for i in range(PARTS):
            rows, low = band(i)
            if spread:
                continue
            ready(i)
            start(has_down, DOWN, i)
        for i in range(PARTS):
            rows, low = band(i)
            if spread:
                continue
            got(has_left, RIGHT_TOP, i)
            got(has_up, DOWN, i)
            out_ref[:, rows] = ext_ref[0, :, rows] - step_size * (
                (tot_ref[0, :, rows] + side_scr[:, rows]) + above_scr[:, rows]
            )
    else:
        for i in range(PARTS):
            start(has_up, UP, i)
            start(has_left, LEFT, i)
        spot = lax.broadcasted_iota(jnp.int32, (t, t), 1)
        spot = jnp.where(spot < t // 2, 2 * spot, 2 * spot - (t - 1))
        perm = jnp.where(lax.broadcasted_iota(jnp.int32, (t, t), 0) == spot, 1.0, 0.0)
        perm_scr[0] = perm.astype(jnp.bfloat16)
        spot = lax.broadcasted_iota(jnp.int32, (t, t), 0)
        spot = jnp.where(spot < t // 2, 2 * spot, 2 * spot - (t - 1))
        perm = jnp.where(lax.broadcasted_iota(jnp.int32, (t, t), 1) == spot, 1.0, 0.0)
        perm_scr[1] = perm.astype(jnp.bfloat16)
        measured.wait()
        slots = amp_ref.shape[0]
        done = 0
        for i in range(PARTS):
            until = min(slots, -(-slots * (i + 1) // (PARTS - 2)))

            def one(s, carry):
                cols = exact(amp_scr[s], lambda piece: dot(piece, perm_scr[0]))
                sorted_ref[s] = exact(cols, lambda piece: dot(perm_scr[1], piece))
                return carry

            lax.fori_loop(done, until, one, 0)
            done = until
            got(has_down, UP, i)
            start(both, LEFT_LOW, i)
    if not reduce:
        own.wait()
        for hold in holds:
            hold.wait()
    if spread:
        for i in range(PARTS):
            got(has_right, LEFT, i)
            got(jnp.logical_and(has_right, has_down), LEFT_LOW, i)
    round_parts = [i for i in range(PARTS) if goes_round(i)]
    plain_parts = [i for i in range(PARTS) if not goes_round(i)]
    if reduce:
        sent(has_right, RIGHT_LOW)
        sent(has_right, RIGHT_TOP)
        sent(has_down, DOWN, plain_parts)
    if folded:
        sent(but(has_down, far_down), DOWN, round_parts)
        sent(far_down, DOWN_VIA, round_parts)
        sent(relay_down, DOWN_ON, round_parts)
        sent(but(has_up, far_up), UP, round_parts)
        sent(far_up, UP_VIA, round_parts)
        sent(relay_up, UP_ON, round_parts)
    if spread:
        sent(has_up, UP, plain_parts)
        sent(has_left, LEFT)
        sent(both, LEFT_LOW)


def exchange(mode, *operands):
    planes, t = operands[0].shape[-3], operands[0].shape[-1]
    vmem = pl.BlockSpec(memory_space=pltpu.VMEM)
    tile = jax.ShapeDtypeStruct((planes, t, t), jnp.float32)
    shapes = [tile if mode == "reduce" else jax.ShapeDtypeStruct((2, planes, 2 * t, t), jnp.float32)]
    specs = [vmem] * len(operands)
    if mode == "spread":
        amp = operands[1]
        specs = [pl.BlockSpec(memory_space=pltpu.HBM)] * 4
        shapes.append(jax.ShapeDtypeStruct(amp.shape, jnp.float32))
        shapes += [jax.ShapeDtypeStruct(table.shape, table.dtype) for table in operands[2:]]
        scratch = [
            pltpu.VMEM(amp.shape, jnp.float32),
            pltpu.VMEM((2, t, t), jnp.bfloat16),
            pltpu.SemaphoreType.DMA((4,)),
        ]
    else:
        scratch = [pltpu.VMEM((planes, 2 * t, t), jnp.float32)]
        scratch += [pltpu.VMEM((planes, t, t), jnp.float32)] * (5 if mode == "both" else 3)
    scratch += [pltpu.SemaphoreType.DMA((10, PARTS))] * 2
    kernel = functools.partial(
        exchange_kernel, mode, lax.axis_size("row"), lax.axis_size("col")
    )
    return pl.pallas_call(
        kernel,
        out_shape=shapes,
        in_specs=specs,
        out_specs=[vmem] * len(shapes),
        scratch_shapes=scratch,
        compiler_params=pltpu.CompilerParams(
            collective_id=("spread", "both", "reduce").index(mode),
            has_side_effects=True,
            vmem_limit_bytes=24 * 1024 * 1024,
        ),
        name="exchange_" + mode,
    )(*operands)


def tables(width):
    half = width // 2
    ladder = np.arange(width)
    theta = (ladder[:, None] * ladder[None, :] % width) * (2.0 * math.pi / width)
    factor = 1.0 / math.sqrt(width)
    cosine = np.cos(theta) * factor
    sine = np.sin(theta) * factor
    out = []
    for parity in (0, 1):
        c = cosine[parity::2, :half]
        s = sine[parity::2, :half]
        out.append(np.block([[c, s], [-s, c]]))
    stacked = np.stack(out).astype(np.float32)
    fwd = jnp.asarray(stacked).astype(jnp.bfloat16)
    inv = jnp.asarray(np.ascontiguousarray(stacked.transpose(0, 2, 1))).astype(jnp.bfloat16)
    return fwd, inv


def dot(a, b):
    return jnp.dot(a, b, preferred_element_type=jnp.float32)


ROWS_OF_CHUNK = 16


def interleave(first, second):
    out, total = [], len(first) + len(second)
    i = j = 0
    for _ in range(total):
        if j >= len(second) or (i < len(first) and i * len(second) <= j * len(first)):
            out.append(first[i])
            i += 1
        else:
            out.append(second[j])
            j += 1
    return out


class Chunks:
    def __init__(self, refs):
        self.free = [list(refs[0]), list(refs[1])]
        self.held = {}

    def feed(self, unit, key, lhs, staged=None):
        ref = self.free[unit].pop(0)
        self.held[unit, key] = ref
        pltpu.matmul_acc_lhs(ref, lhs, load_staged_rhs=staged)

    def pop(self, unit, key):
        ref = self.held.pop((unit, key))
        self.free[unit].append(ref)
        return pltpu.matmul_pop(ref)


class Step:
    def __init__(self, refs, acc):
        self.__dict__.update(refs)
        self.acc = acc
        self.modes, _, self.width, _ = self.probe.shape
        self.h = self.width // 2
        self.flip = 0

    def corner(self, s):
        lane, sub = 128, 8
        top, left = self.pos[0, s], self.pos[1, s]
        base = left // lane
        rest = left - base * lane
        over = pl.multiple_of((top // sub) * sub, sub)
        return base, rest, over, top - over

    def block_of(self, base, c):
        lane = 128
        per = self.width // lane
        half = (base + c) // per
        near = base + c - half * per
        return half, pl.ds(pl.multiple_of(near * lane, lane), lane)

    def cut_patch(self, s):
        lane, sub, width = 128, 8, self.width
        base, rest, over, drop = self.corner(s)
        part = 64
        units = []
        lanes = lax.broadcasted_iota(jnp.int32, (part, lane), 1)
        ledge = lax.broadcasted_iota(jnp.int32, (part // sub, sub, lane), 1)

        def unit(d, r):
            turned = []
            for c in range(width // lane + 1):
                half, cols = self.block_of(base, c)
                rows = pl.ds(pl.multiple_of(over + r, sub), part + sub)
                x = self.ext[half, d, rows, cols].reshape(part // sub + 1, sub, lane)
                x = pltpu.roll(x, lax.rem(sub - drop, sub), 1)
                x = jnp.where(ledge + drop < sub, x[:-1], x[1:]).reshape(part, lane)
                turned.append(pltpu.roll(x, lax.rem(lane - rest, lane), 1))
            for c in range(width // lane):
                self.patch[d, r : r + part, c * lane : (c + 1) * lane] = jnp.where(
                    lanes + rest < lane, turned[c], turned[c + 1]
                )

        for r in range(0, width, part):
            for d in range(2):
                units.append(functools.partial(unit, d, r))
        return units

    def make_psi(self, m):
        h, step = self.h, 16
        out = self.psi.at[m % 2]

        def unit(r):
            rows, low = slice(r, r + step), slice(h + r, h + r + step)
            pr, pi = self.probe[m, 0, rows], self.probe[m, 1, rows]
            qr, qi = self.probe[m, 0, low], self.probe[m, 1, low]
            fr, fi = self.patch[0, rows], self.patch[1, rows]
            gr, gi = self.patch[0, low], self.patch[1, low]
            ur, ui = pr * fr - pi * fi, pr * fi + pi * fr
            vr, vi = qr * gr - qi * gi, qr * gi + qi * gr
            out[0, rows] = (ur + vr).astype(jnp.bfloat16)
            out[0, low] = (ui + vi).astype(jnp.bfloat16)
            out[1, rows] = (ur - vr).astype(jnp.bfloat16)
            out[1, low] = (ui - vi).astype(jnp.bfloat16)

        return [functools.partial(unit, r) for r in range(0, h, step)]

    def weigh(self, m, s):
        n, h = ROWS_OF_CHUNK, self.h

        def unit(q, r):
            rows = slice(r, r + n)
            far = self.acc.pop(q, ("R1", m, r))
            self.far[m, q, rows] = far
            re, im = far[:, :h], far[:, h:]
            term = re * re + im * im
            if m > 0:
                term = self.bright[q, rows] + term
            if m < self.modes - 1:
                self.bright[q, rows] = term
            else:
                seen = self.amp[s, rows, q * h : (q + 1) * h]
                self.ratio[q, rows] = 1.0 - seen * lax.rsqrt(term + damping)

        return [functools.partial(unit, q, r) for r in range(0, self.width, n) for q in range(2)]

    def make_chi(self, m):
        n, h = ROWS_OF_CHUNK, self.h
        out = self.chi.at[m % 2]

        def unit(p, r):
            for q in range(2):
                cols = slice(q * h, (q + 1) * h)
                rows = slice(p * h + r, p * h + r + n)
                ratio = self.ratio[q, rows]
                out[p, r : r + n, cols] = (self.far[m, q, rows, :h] * ratio).astype(jnp.bfloat16)
                out[p, h + r : h + r + n, cols] = (self.far[m, q, rows, h:] * ratio).astype(
                    jnp.bfloat16
                )

        return [functools.partial(unit, p, r) for r in range(0, h, n) for p in range(2)]

    def gather(self, m):
        n, h = ROWS_OF_CHUNK, self.h

        def unit(r):
            rows = slice(r, r + n)
            even, odd = self.acc.pop(0, ("R2", m, r)), self.acc.pop(1, ("R2", m, r))
            for cols, wave in ((slice(0, h), even + odd), (slice(h, 2 * h), even - odd)):
                wr, wi = wave[:, :h], wave[:, h:]
                pr, pi = self.probe[m, 0, rows, cols], self.probe[m, 1, rows, cols]
                gr, gi = pr * wr + pi * wi, pr * wi - pi * wr
                if m > 0:
                    gr, gi = self.grad[0, rows, cols] + gr, self.grad[1, rows, cols] + gi
                self.grad[0, rows, cols] = gr
                self.grad[1, rows, cols] = gi

        return [functools.partial(unit, r) for r in range(0, self.width, n)]

    def place(self, s):
        lane, sub, width = 128, 8, self.width
        base, rest, over, drop = self.corner(s)
        wide = width // lane + 1
        blocks = width // sub
        part = 64
        lanes = lax.broadcasted_iota(jnp.int32, (part, lane), 1)

        def unit(d, r):
            edge = jnp.zeros((part, lane), jnp.float32)
            turned = [edge]
            for c in range(width // lane):
                x = self.grad[d, r : r + part, c * lane : (c + 1) * lane]
                turned.append(pltpu.roll(x, rest, 1))
            turned.append(edge)
            for c in range(wide):
                x = jnp.where(lanes >= rest, turned[c + 1], turned[c])
                x = pltpu.roll(x.reshape(part // sub, sub, lane), drop, 1)
                brim = jnp.zeros((1, sub, lane), jnp.float32)
                after = jnp.concatenate([x, brim], axis=0)
                before = jnp.concatenate([brim, x], axis=0)
                rim = lax.broadcasted_iota(jnp.int32, (part // sub + 1, sub, lane), 1)
                x = jnp.where(rim >= drop, after, before).reshape(part + sub, lane)
                half, cols = self.block_of(base, c)
                spot = (half, d, pl.ds(pl.multiple_of(over + r, sub), part + sub), cols)
                self.tot[spot] = self.tot[spot] + x

        return [functools.partial(unit, d, r) for r in range(0, width, part) for d in range(2)]

    def left(self, kind, m):
        n, h = ROWS_OF_CHUNK, self.h
        rhs, lhs = (self.psi, self.a) if kind == "L1" else (self.chi, self.b)
        reg = self.flip
        self.flip = 1 - reg

        def push():
            for unit in range(2):
                pltpu.matmul_push_rhs(rhs[m % 2, unit], reg, unit)

        def feed(r, first):
            for unit in range(2):
                self.acc.feed(unit, (kind, m, r), lhs[unit, r : r + n], reg if first else None)

        order = [r + d for r in range(0, h, n) for d in (0, h)]
        return push, [functools.partial(feed, r, k == 0) for k, r in enumerate(order)]

    def right(self, kind, m):
        n, h = ROWS_OF_CHUNK, self.h
        rhs = self.b if kind == "R1" else self.a
        reg = self.flip
        self.flip = 1 - reg

        def push():
            for unit in range(2):
                pltpu.matmul_push_rhs(rhs[unit], reg, unit)

        def feed_forward(r, p, first):
            re, im = self.acc.pop(p, ("L1", m, r)), self.acc.pop(p, ("L1", m, h + r))
            re_l, re_r, im_l, im_r = re[:, :h], re[:, h:], im[:, :h], im[:, h:]
            plus = jnp.concatenate([re_l + re_r, im_l + im_r], axis=1).astype(jnp.bfloat16)
            less = jnp.concatenate([re_l - re_r, im_l - im_r], axis=1).astype(jnp.bfloat16)
            for unit, x in enumerate((plus, less)):
                self.acc.feed(unit, (kind, m, p * h + r), x, reg if first else None)

        def feed_backward(r, first):
            key = ("L2", m, r), ("L2", m, h + r)
            ere, oim = self.acc.pop(0, key[0]), self.acc.pop(1, key[1])
            ore, eim = self.acc.pop(1, key[0]), self.acc.pop(0, key[1])
            for k, (re, im) in enumerate(((ere + ore, eim + oim), (ere - ore, eim - oim))):
                for unit in range(2):
                    cols = slice(unit * h, (unit + 1) * h)
                    y = jnp.concatenate([re[:, cols], im[:, cols]], axis=1).astype(jnp.bfloat16)
                    self.acc.feed(
                        unit, (kind, m, k * h + r), y, reg if first and k == 0 else None
                    )

        if kind == "R1":
            spots = [(r, p) for r in range(0, h, n) for p in range(2)]
            feeds = [functools.partial(feed_forward, r, p, k == 0) for k, (r, p) in enumerate(spots)]
        else:
            feeds = [functools.partial(feed_backward, r, r == 0) for r in range(0, h, n)]
        return push, feeds

    def run(self, jobs):
        built = []
        for kind, m, beside in jobs:
            if kind is None:
                built.append((None, [], beside))
                continue
            push, feeds = (self.left if kind[0] == "L" else self.right)(kind, m)
            built.append((push, feeds, beside))
        for k, (push, feeds, beside) in enumerate(built):
            if push is not None and (k == 0 or built[k - 1][0] is None):
                push()
            for unit in interleave(beside, feeds):
                unit()
            if push is not None and k + 1 < len(built) and built[k + 1][0] is not None:
                built[k + 1][0]()


def forward_only(step, s, ahead, blank):
    psi, weigh = step.make_psi, lambda m: step.weigh(m, s)
    for unit in step.cut_patch(s) + psi(0):
        unit()
    step.run(
        [
            ("L1", 0, psi(1)),
            ("L1", 1, psi(2)),
            ("R1", 0, psi(3)),
            ("L1", 2, weigh(0)),
            ("R1", 1, step.cut_patch(ahead)),
            ("L1", 3, weigh(1) + blank[:16]),
            ("R1", 2, psi(0) + blank[16:]),
            ("R1", 3, weigh(2)),
            (None, 0, weigh(3)),
        ]
    )


def backward_only(step, s, behind):
    chi, gather, place = step.make_chi, step.gather, step.place(behind)
    half = len(place) // 2
    step.run(
        [
            (None, 0, chi(0)),
            ("L2", 0, chi(1) + place[:half]),
            ("L2", 1, chi(2) + place[half:]),
            ("R2", 0, []),
            ("L2", 2, chi(3) + gather(0)),
            ("R2", 1, []),
            ("L2", 3, gather(1)),
            ("R2", 2, []),
            ("R2", 3, gather(2)),
            (None, 0, gather(3) + step.place(s)),
        ]
    )


def both_ways(step, behind, back, ahead, beyond):
    psi, weigh = step.make_psi, lambda m: step.weigh(m, ahead)
    chi, gather = step.make_chi, step.gather
    cut, place = step.cut_patch(beyond), step.place(behind)
    psi1, psi2, psi3, psi0 = psi(1), psi(2), psi(3), psi(0)
    step.run(
        [
            ("L1", 0, interleave(chi(0), psi1[:3])),
            ("L2", 0, interleave(chi(1), psi1[3:])),
            ("L1", 1, place[:5]),
            ("R2", 0, place[5:]),
            ("L2", 1, psi2),
            ("R1", 0, gather(0)),
            ("R2", 1, chi(2)),
            ("L2", 2, interleave(chi(3), weigh(0))),
            ("L1", 2, psi3),
            ("R2", 2, gather(1)),
            ("L2", 3, cut),
            ("R1", 1, gather(2)),
            ("L1", 3, weigh(1)),
            ("R2", 3, psi0),
            ("R1", 2, []),
            ("R1", 3, interleave(gather(3), weigh(2))),
            (None, 0, weigh(3)),
        ]
    )


NAMES = ("count", "pos", "ext", "amp", "probe", "a", "b", "tot")
NAMES += ("patch", "psi", "far", "chi", "grad", "bright", "ratio")


def gradient_kernel(*operands):
    refs = dict(zip(NAMES, operands))
    tot = refs["tot"]

    def clear(half, d, r):
        part = 64
        tot[half, d, r : r + part] = jnp.zeros((part, tot.shape[3]), jnp.float32)

    blank = [
        functools.partial(clear, half, d, r)
        for half in range(2)
        for d in range(2)
        for r in range(0, tot.shape[2], 64)
    ]
    refs["grad"][...] = jnp.zeros_like(refs["grad"])
    count = refs["count"][0, 0]
    last = refs["amp"].shape[0] - 1

    def with_units(work, *where):
        def body(*acc):
            half = len(acc) // 2
            work(Step(refs, Chunks((acc[:half], acc[half:]))), *where)

        depth = 1024 // ROWS_OF_CHUNK
        shape = (ROWS_OF_CHUNK, refs["probe"].shape[-1])
        pl.run_scoped(body, *[pltpu.ACC(u)(shape, jnp.float32) for u in (0, 1) for _ in range(depth)])

    @pl.when(count > 0)
    def _():
        with_units(forward_only, 0, min(1, last), blank)

    @pl.when(count <= 0)
    def _():
        for unit in blank:
            unit()

    def one(s, carry):
        with_units(both_ways, jnp.maximum(s - 1, 0), s, s + 1, jnp.minimum(s + 2, last))
        return carry

    lax.fori_loop(0, count - 1, one, 0)

    @pl.when(count > 0)
    def _():
        with_units(backward_only, count - 1, jnp.maximum(count - 2, 0))


def gradient(counts, where, extended, amp, probe_modes, fwd, inv):
    modes, _, width, _ = probe_modes.shape
    vmem = pl.BlockSpec(memory_space=pltpu.VMEM)
    smem = pl.BlockSpec(memory_space=pltpu.SMEM)
    half = width // 2
    return pl.pallas_call(
        gradient_kernel,
        out_shape=jax.ShapeDtypeStruct(extended.shape, jnp.float32),
        in_specs=[smem, smem] + [vmem] * 5,
        out_specs=vmem,
        scratch_shapes=[
            pltpu.VMEM((2, width, width), jnp.float32),
            pltpu.VMEM((2, 2, width, width), jnp.bfloat16),
            pltpu.VMEM((modes, 2, width, width), jnp.float32),
            pltpu.VMEM((2, 2, width, width), jnp.bfloat16),
            pltpu.VMEM((2, width, width), jnp.float32),
            pltpu.VMEM((2, width, half), jnp.float32),
            pltpu.VMEM((2, width, half), jnp.float32),
        ],
        compiler_params=pltpu.CompilerParams(vmem_limit_bytes=40 * 1024 * 1024),
        name="gradient",
    )(counts, where, extended, amp, probe_modes, fwd, inv)


def exact(values, product):
    total = None
    for _ in range(3):
        piece = values.astype(jnp.bfloat16)
        values = values - piece.astype(jnp.float32)
        part = product(piece)
        total = part if total is None else total + part
    return total


def body(object_field, probe_modes, positions, counts, amplitude):
    width = probe_modes.shape[-1]
    fwd, inv = tables(width)
    where = positions[0, 0].T
    held = [
        pltpu.with_memory_space_constraint(x, pltpu.HBM)
        for x in (object_field, amplitude[0, 0], fwd, inv)
    ]
    extended, amp, fwd, inv = exchange("spread", *held)
    for sweep in range(ITERS):
        total = gradient(counts, where, extended, amp, probe_modes, fwd, inv)
        (extended,) = exchange("both" if sweep < ITERS - 1 else "reduce", total, extended)
    return extended


def solution(mesh):
    placed = (
        P(None, "row", "col"),
        P(),
        P("row", "col", None, None),
        P("row", "col"),
        P("row", "col", None, None, None),
    )
    return jax.shard_map(
        body, mesh=mesh, in_specs=placed, out_specs=P(None, "row", "col"), check_vma=False
    )
```

```python
import functools
import math

import jax
import jax.numpy as jnp
import numpy as np
from jax import lax
from jax.experimental import pallas as pl
from jax.experimental.pallas import tpu as pltpu
from jax.sharding import PartitionSpec as P

ITERS = 2


step_size = 0.1
damping = 0.1


RIGHT_LOW, RIGHT_TOP, DOWN, UP, LEFT, LEFT_LOW = range(6)
UP_VIA, UP_ON, DOWN_VIA, DOWN_ON = range(6, 10)
DIAG = 10
SHARES = (9, 10, 8, 5)
SPREAD_SHARES = (11, 10, 6, 5)
PARTS = len(SHARES)


def exchange_kernel(mode, rows_of, cols_of, *refs):
    refs = list(refs)
    reduce, spread = mode != "spread", mode != "reduce"
    if reduce:
        tot_ref, ext_ref, out_ref = refs.pop(0), refs.pop(0), refs.pop(0)
        side_scr, top_scr, low_scr, above_scr = [refs.pop(0) for _ in range(4)]
        below_scr = refs.pop(0) if spread else None
        via_scr = refs.pop(0) if spread else None
        t = out_ref.shape[-1]
    else:
        field_ref, amp_ref, *table_refs = [refs.pop(0) for _ in range(4)]
        out_ref, sorted_ref, *held_refs = [refs.pop(0) for _ in range(4)]
        amp_scr, perm_scr, local_sem = [refs.pop(0) for _ in range(3)]
        t = field_ref.shape[-1]
    send_sem, recv_sem = refs
    shares = SHARES if reduce else SPREAD_SHARES
    unit = t // sum(shares)
    starts = [sum(shares[:i]) * unit for i in range(PARTS)]
    sizes = [share * unit for share in shares]
    last = PARTS - 1
    r, c = lax.axis_index("row"), lax.axis_index("col")
    has_up, has_down = r > 0, r < rows_of - 1
    has_left, has_right = c > 0, c < cols_of - 1
    up = (jnp.where(has_up, r - 1, r + 1), c)
    down = (jnp.where(has_down, r + 1, r - 1), c)
    left = (r, jnp.where(has_left, c - 1, c + 1))
    right = (r, jnp.where(has_right, c + 1, c - 1))
    folded = reduce and spread and rows_of % 2 == 0 and rows_of > 2
    even, odd = lax.rem(r, 2) == 0, lax.rem(r, 2) == 1
    has_up2, has_down2 = r > 1, r < rows_of - 2
    up2 = (jnp.where(has_up2, r - 2, r + 2), c)
    down2 = (jnp.where(has_down2, r + 2, r - 2), c)
    far_up, far_down = jnp.logical_and(even, has_up), jnp.logical_and(odd, has_down)
    relay_up, relay_down = jnp.logical_and(even, has_down2), jnp.logical_and(odd, has_up2)

    def goes_round(i):
        return folded and i % 2 == 0

    def but(a, b):
        return jnp.logical_and(a, jnp.logical_not(b))

    if not reduce:
        own = pltpu.make_async_copy(field_ref, out_ref.at[0, :, pl.ds(0, t)], local_sem.at[0])
        own.start()
        measured = pltpu.make_async_copy(amp_ref, amp_scr, local_sem.at[1])
        measured.start()
        holds = [
            pltpu.make_async_copy(table_refs[k], held_refs[k], local_sem.at[2 + k]) for k in range(2)
        ]
        for hold in holds:
            hold.start()

    barrier = pltpu.get_barrier_semaphore()
    peers_of = [(has_up, up), (has_down, down), (has_left, left), (has_right, right)]
    if folded:
        peers_of += [(has_up2, up2), (has_down2, down2)]
    for there, device in peers_of:

        @pl.when(there)
        def _():
            pl.semaphore_signal(
                barrier, inc=1, device_id=device, device_id_type=pl.DeviceIdType.MESH
            )

    peers = sum(jnp.where(there, 1, 0) for there, _ in peers_of)
    pl.semaphore_wait(barrier, peers)

    def copy(kind, i):
        rows = pl.ds(starts[i], sizes[i])
        low = pl.ds(t + starts[i], sizes[i])
        if kind == RIGHT_LOW:
            src, dst, device = tot_ref.at[1, :, low], side_scr.at[:, low], right
        elif kind == RIGHT_TOP:
            src, dst, device = tot_ref.at[1, :, rows], side_scr.at[:, rows], right
        elif kind == DOWN:
            src, dst, device = low_scr.at[:, rows], above_scr.at[:, rows], down
        elif kind == UP and reduce:
            src, dst, device = top_scr.at[:, rows], below_scr.at[:, rows], up
        elif kind == UP:
            src, dst, device = field_ref.at[:, rows], out_ref.at[0, :, low], up
        elif kind == UP_VIA:
            src, dst, device = top_scr.at[:, rows], via_scr.at[:, rows], up2
        elif kind == UP_ON:
            src, dst, device = via_scr.at[:, rows], below_scr.at[:, rows], down
        elif kind == DOWN_VIA:
            src, dst, device = low_scr.at[:, rows], via_scr.at[:, rows], down2
        elif kind == DOWN_ON:
            src, dst, device = via_scr.at[:, rows], above_scr.at[:, rows], up
        elif kind == DIAG:
            src, dst, device = out_ref.at[1, :, rows], out_ref.at[1, :, low], up
        elif kind == LEFT and reduce:
            src, dst, device = out_ref.at[0, :, rows], out_ref.at[1, :, rows], left
        elif kind == LEFT:
            src, dst, device = field_ref.at[:, rows], out_ref.at[1, :, rows], left
        else:
            src, dst, device = out_ref.at[0, :, low], out_ref.at[1, :, low], left
        return pltpu.make_async_remote_copy(
            src_ref=src,
            dst_ref=dst,
            send_sem=send_sem.at[kind, i],
            recv_sem=recv_sem.at[kind, i],
            device_id=device,
            device_id_type=pl.DeviceIdType.MESH,
        )

    def start(there, kind, i):
        @pl.when(there)
        def _():
            copy(kind, i).start()

    def got(there, kind, i):
        @pl.when(there)
        def _():
            copy(kind, i).wait_recv()

    def sent(there, kind, parts=range(PARTS)):
        @pl.when(there)
        def _():
            for i in parts:
                copy(kind, i).wait_send()

    if reduce:
        for i in range(PARTS):
            start(jnp.logical_and(has_right, even) if spread else has_right, RIGHT_LOW, i)
            if spread:
                start(has_right, RIGHT_TOP, i)
                start(jnp.logical_and(has_right, odd), RIGHT_LOW, i)
        if not spread:
            for i in range(PARTS):
                start(has_right, RIGHT_TOP, i)

        @pl.when(jnp.logical_not(has_left))
        def _():
            side_scr[...] = jnp.zeros_like(side_scr)

        @pl.when(jnp.logical_not(has_up))
        def _():
            above_scr[...] = jnp.zeros_like(above_scr)

    if spread:

        @pl.when(jnp.logical_not(has_down))
        def _():
            out_ref[0, :, t:] = jnp.zeros((2, t, t), jnp.float32)

        @pl.when(jnp.logical_not(has_right))
        def _():
            out_ref[1] = jnp.zeros((2, 2 * t, t), jnp.float32)

        @pl.when(jnp.logical_and(has_right, jnp.logical_not(has_down)))
        def _():
            out_ref[1, :, t:] = jnp.zeros((2, t, t), jnp.float32)

    def band(i):
        first, end = starts[i], starts[i] + sizes[i]
        return slice(first, end), slice(t + first, t + end)

    both = jnp.logical_and(has_down, has_left)
    if reduce:
        def ready(i):
            rows, low = band(i)
            got(has_left, RIGHT_LOW, i)

            @pl.when(has_down)
            def _():
                low_scr[:, rows] = tot_ref[0, :, low] + side_scr[:, low]

            if spread:
                got(has_left, RIGHT_TOP, i)
                top_scr[:, rows] = tot_ref[0, :, rows] + side_scr[:, rows]

        def within(i):
            start(jnp.logical_and(odd, has_up), UP, i)
            start(jnp.logical_and(even, has_down), DOWN, i)

        def across(i):
            start(far_up, UP_VIA if goes_round(i) else UP, i)
            start(far_down, DOWN_VIA if goes_round(i) else DOWN, i)

        def pass_on(i):
            got(relay_up, UP_VIA, i)
            start(relay_up, UP_ON, i)
            got(relay_down, DOWN_VIA, i)
            start(relay_down, DOWN_ON, i)

        def own_band(there, i, kinds):
            rows, _ = band(i)

            @pl.when(there)
            def _():
                for also, kind in kinds:
                    got(also, kind, i)
                out_ref[0, :, rows] = ext_ref[0, :, rows] - step_size * (
                    top_scr[:, rows] + above_scr[:, rows]
                )
                start(has_left, LEFT, i)

        def low_band(there, i, kinds):
            rows, low = band(i)

            @pl.when(jnp.logical_and(there, has_down))
            def _():
                for also, kind in kinds:
                    got(also, kind, i)
                out_ref[0, :, low] = ext_ref[0, :, low] - step_size * (
                    low_scr[:, rows] + below_scr[:, rows]
                )
                start(has_left, LEFT_LOW, i)

        def settle_within(i):
            low_band(even, i, [(has_down, UP)])
            own_band(odd, i, [(has_up, DOWN)])

        def settle_across(i):
            own_band(even, i, [(has_up, DOWN_ON if goes_round(i) else DOWN)])
            low_band(odd, i, [(has_down, UP_ON if goes_round(i) else UP)])

        if spread and folded:
            for i in range(0, PARTS, 2):
                ready(i)
                if i > 0:
                    pass_on(i - 2)
                within(i)
                across(i)
                ready(i + 1)
                if i == 0:
                    within(i + 1)
                    across(i + 1)
                else:
                    across(i + 1)
                    within(i + 1)
            late = PARTS - 2
            settle_within(0)
            settle_within(1)
            pass_on(late)
            for i in range(PARTS):
                settle_across(i)
                if i > 0 and i + 1 < PARTS:
                    settle_within(i + 1)
        elif spread:
            for i in range(PARTS):
                ready(i)
                within(i)
                across(i)
            for i in range(PARTS):
                settle_within(i)
                settle_across(i)
        for i in range(PARTS):
            rows, low = band(i)
            if spread:
                continue
            ready(i)
            start(has_down, DOWN, i)
        for i in range(PARTS):
            rows, low = band(i)
            if spread:
                continue
            got(has_left, RIGHT_TOP, i)
            got(has_up, DOWN, i)
            out_ref[:, rows] = ext_ref[0, :, rows] - step_size * (
                (tot_ref[0, :, rows] + side_scr[:, rows]) + above_scr[:, rows]
            )
    else:
        for i in range(PARTS):
            start(has_up, UP, i)
            start(has_left, LEFT, i)
        spot = lax.broadcasted_iota(jnp.int32, (t, t), 1)
        spot = jnp.where(spot < t // 2, 2 * spot, 2 * spot - (t - 1))
        perm = jnp.where(lax.broadcasted_iota(jnp.int32, (t, t), 0) == spot, 1.0, 0.0)
        perm_scr[0] = perm.astype(jnp.bfloat16)
        spot = lax.broadcasted_iota(jnp.int32, (t, t), 0)
        spot = jnp.where(spot < t // 2, 2 * spot, 2 * spot - (t - 1))
        perm = jnp.where(lax.broadcasted_iota(jnp.int32, (t, t), 1) == spot, 1.0, 0.0)
        perm_scr[1] = perm.astype(jnp.bfloat16)
        measured.wait()
        slots = amp_ref.shape[0]
        done = 0
        for i in range(PARTS):
            until = min(slots, -(-slots * (i + 1) // (PARTS - 2)))

            def one(s, carry):
                cols = exact(amp_scr[s], lambda piece: dot(piece, perm_scr[0]))
                sorted_ref[s] = exact(cols, lambda piece: dot(perm_scr[1], piece))
                return carry

            lax.fori_loop(done, until, one, 0)
            done = until
            got(has_down, UP, i)
            if i < last:
                start(both, LEFT_LOW, i)
            if i == 0:
                got(has_right, LEFT, last)
                start(jnp.logical_and(has_right, has_up), DIAG, last)
    if not reduce:
        own.wait()
        for hold in holds:
            hold.wait()
    if spread:
        for i in range(PARTS):
            ahead = not reduce and i == last
            if not ahead:
                got(has_right, LEFT, i)
            got(jnp.logical_and(has_right, has_down), DIAG if ahead else LEFT_LOW, i)
    round_parts = [i for i in range(PARTS) if goes_round(i)]
    plain_parts = [i for i in range(PARTS) if not goes_round(i)]
    if reduce:
        sent(has_right, RIGHT_LOW)
        sent(has_right, RIGHT_TOP)
        sent(has_down, DOWN, plain_parts)
    if folded:
        sent(but(has_down, far_down), DOWN, round_parts)
        sent(far_down, DOWN_VIA, round_parts)
        sent(relay_down, DOWN_ON, round_parts)
        sent(but(has_up, far_up), UP, round_parts)
        sent(far_up, UP_VIA, round_parts)
        sent(relay_up, UP_ON, round_parts)
    if spread:
        sent(has_up, UP, plain_parts)
        sent(has_left, LEFT)
        sent(both, LEFT_LOW, range(PARTS if reduce else last))
        if not reduce:
            sent(jnp.logical_and(has_right, has_up), DIAG, [last])


def exchange(mode, *operands):
    planes, t = operands[0].shape[-3], operands[0].shape[-1]
    vmem = pl.BlockSpec(memory_space=pltpu.VMEM)
    tile = jax.ShapeDtypeStruct((planes, t, t), jnp.float32)
    shapes = [tile if mode == "reduce" else jax.ShapeDtypeStruct((2, planes, 2 * t, t), jnp.float32)]
    specs = [vmem] * len(operands)
    if mode == "spread":
        amp = operands[1]
        specs = [pl.BlockSpec(memory_space=pltpu.HBM)] * 4
        shapes.append(jax.ShapeDtypeStruct(amp.shape, jnp.float32))
        shapes += [jax.ShapeDtypeStruct(table.shape, table.dtype) for table in operands[2:]]
        scratch = [
            pltpu.VMEM(amp.shape, jnp.float32),
            pltpu.VMEM((2, t, t), jnp.bfloat16),
            pltpu.SemaphoreType.DMA((4,)),
        ]
    else:
        scratch = [pltpu.VMEM((planes, 2 * t, t), jnp.float32)]
        scratch += [pltpu.VMEM((planes, t, t), jnp.float32)] * (5 if mode == "both" else 3)
    scratch += [pltpu.SemaphoreType.DMA((11, PARTS))] * 2
    kernel = functools.partial(
        exchange_kernel, mode, lax.axis_size("row"), lax.axis_size("col")
    )
    return pl.pallas_call(
        kernel,
        out_shape=shapes,
        in_specs=specs,
        out_specs=[vmem] * len(shapes),
        scratch_shapes=scratch,
        compiler_params=pltpu.CompilerParams(
            collective_id=("spread", "both", "reduce").index(mode),
            has_side_effects=True,
            vmem_limit_bytes=24 * 1024 * 1024,
        ),
        name="exchange_" + mode,
    )(*operands)


def tables(width):
    half = width // 2
    ladder = np.arange(width)
    theta = (ladder[:, None] * ladder[None, :] % width) * (2.0 * math.pi / width)
    factor = 1.0 / math.sqrt(width)
    cosine = np.cos(theta) * factor
    sine = np.sin(theta) * factor
    out = []
    for parity in (0, 1):
        c = cosine[parity::2, :half]
        s = sine[parity::2, :half]
        out.append(np.block([[c, s], [-s, c]]))
    stacked = np.stack(out).astype(np.float32)
    fwd = jnp.asarray(stacked).astype(jnp.bfloat16)
    inv = jnp.asarray(np.ascontiguousarray(stacked.transpose(0, 2, 1))).astype(jnp.bfloat16)
    return fwd, inv


def dot(a, b):
    return jnp.dot(a, b, preferred_element_type=jnp.float32)


ROWS_OF_CHUNK = 16


def interleave(first, second):
    out, total = [], len(first) + len(second)
    i = j = 0
    for _ in range(total):
        if j >= len(second) or (i < len(first) and i * len(second) <= j * len(first)):
            out.append(first[i])
            i += 1
        else:
            out.append(second[j])
            j += 1
    return out


class Chunks:
    def __init__(self, refs):
        self.free = [list(refs[0]), list(refs[1])]
        self.held = {}

    def feed(self, unit, key, lhs, staged=None):
        ref = self.free[unit].pop(0)
        self.held[unit, key] = ref
        pltpu.matmul_acc_lhs(ref, lhs, load_staged_rhs=staged)

    def pop(self, unit, key):
        ref = self.held.pop((unit, key))
        self.free[unit].append(ref)
        return pltpu.matmul_pop(ref)


class Step:
    def __init__(self, refs, acc):
        self.__dict__.update(refs)
        self.acc = acc
        self.modes, _, self.width, _ = self.probe.shape
        self.h = self.width // 2
        self.flip = 0

    def corner(self, s):
        lane, sub = 128, 8
        top, left = self.pos[0, s], self.pos[1, s]
        base = left // lane
        rest = left - base * lane
        over = pl.multiple_of((top // sub) * sub, sub)
        return base, rest, over, top - over

    def block_of(self, base, c):
        lane = 128
        per = self.width // lane
        half = (base + c) // per
        near = base + c - half * per
        return half, pl.ds(pl.multiple_of(near * lane, lane), lane)

    def cut_patch(self, s):
        lane, sub, width = 128, 8, self.width
        base, rest, over, drop = self.corner(s)
        part = 64
        units = []
        lanes = lax.broadcasted_iota(jnp.int32, (part, lane), 1)
        ledge = lax.broadcasted_iota(jnp.int32, (part // sub, sub, lane), 1)

        def unit(d, r):
            turned = []
            for c in range(width // lane + 1):
                half, cols = self.block_of(base, c)
                rows = pl.ds(pl.multiple_of(over + r, sub), part + sub)
                x = self.ext[half, d, rows, cols].reshape(part // sub + 1, sub, lane)
                x = pltpu.roll(x, lax.rem(sub - drop, sub), 1)
                x = jnp.where(ledge + drop < sub, x[:-1], x[1:]).reshape(part, lane)
                turned.append(pltpu.roll(x, lax.rem(lane - rest, lane), 1))
            for c in range(width // lane):
                self.patch[d, r : r + part, c * lane : (c + 1) * lane] = jnp.where(
                    lanes + rest < lane, turned[c], turned[c + 1]
                )

        for r in range(0, width, part):
            for d in range(2):
                units.append(functools.partial(unit, d, r))
        return units

    def make_psi(self, m):
        h, step = self.h, 16
        out = self.psi.at[m % 2]

        def unit(r):
            rows, low = slice(r, r + step), slice(h + r, h + r + step)
            pr, pi = self.probe[m, 0, rows], self.probe[m, 1, rows]
            qr, qi = self.probe[m, 0, low], self.probe[m, 1, low]
            fr, fi = self.patch[0, rows], self.patch[1, rows]
            gr, gi = self.patch[0, low], self.patch[1, low]
            ur, ui = pr * fr - pi * fi, pr * fi + pi * fr
            vr, vi = qr * gr - qi * gi, qr * gi + qi * gr
            out[0, rows] = (ur + vr).astype(jnp.bfloat16)
            out[0, low] = (ui + vi).astype(jnp.bfloat16)
            out[1, rows] = (ur - vr).astype(jnp.bfloat16)
            out[1, low] = (ui - vi).astype(jnp.bfloat16)

        return [functools.partial(unit, r) for r in range(0, h, step)]

    def weigh(self, m, s):
        n, h = ROWS_OF_CHUNK, self.h

        def unit(q, r):
            rows = slice(r, r + n)
            far = self.acc.pop(q, ("R1", m, r))
            self.far[m, q, rows] = far
            re, im = far[:, :h], far[:, h:]
            term = re * re + im * im
            if m > 0:
                term = self.bright[q, rows] + term
            if m < self.modes - 1:
                self.bright[q, rows] = term
            else:
                seen = self.amp[s, rows, q * h : (q + 1) * h]
                self.ratio[q, rows] = 1.0 - seen * lax.rsqrt(term + damping)

        return [functools.partial(unit, q, r) for r in range(0, self.width, n) for q in range(2)]

    def make_chi(self, m):
        n, h = ROWS_OF_CHUNK, self.h
        out = self.chi.at[m % 2]

        def unit(p, r):
            for q in range(2):
                cols = slice(q * h, (q + 1) * h)
                rows = slice(p * h + r, p * h + r + n)
                ratio = self.ratio[q, rows]
                out[p, r : r + n, cols] = (self.far[m, q, rows, :h] * ratio).astype(jnp.bfloat16)
                out[p, h + r : h + r + n, cols] = (self.far[m, q, rows, h:] * ratio).astype(
                    jnp.bfloat16
                )

        return [functools.partial(unit, p, r) for r in range(0, h, n) for p in range(2)]

    def gather(self, m):
        n, h = ROWS_OF_CHUNK, self.h

        def unit(r):
            rows = slice(r, r + n)
            even, odd = self.acc.pop(0, ("R2", m, r)), self.acc.pop(1, ("R2", m, r))
            for cols, wave in ((slice(0, h), even + odd), (slice(h, 2 * h), even - odd)):
                wr, wi = wave[:, :h], wave[:, h:]
                pr, pi = self.probe[m, 0, rows, cols], self.probe[m, 1, rows, cols]
                gr, gi = pr * wr + pi * wi, pr * wi - pi * wr
                if m > 0:
                    gr, gi = self.grad[0, rows, cols] + gr, self.grad[1, rows, cols] + gi
                self.grad[0, rows, cols] = gr
                self.grad[1, rows, cols] = gi

        return [functools.partial(unit, r) for r in range(0, self.width, n)]

    def place(self, s):
        lane, sub, width = 128, 8, self.width
        base, rest, over, drop = self.corner(s)
        wide = width // lane + 1
        blocks = width // sub
        part = 64
        lanes = lax.broadcasted_iota(jnp.int32, (part, lane), 1)

        def unit(d, r):
            edge = jnp.zeros((part, lane), jnp.float32)
            turned = [edge]
            for c in range(width // lane):
                x = self.grad[d, r : r + part, c * lane : (c + 1) * lane]
                turned.append(pltpu.roll(x, rest, 1))
            turned.append(edge)
            for c in range(wide):
                x = jnp.where(lanes >= rest, turned[c + 1], turned[c])
                x = pltpu.roll(x.reshape(part // sub, sub, lane), drop, 1)
                brim = jnp.zeros((1, sub, lane), jnp.float32)
                after = jnp.concatenate([x, brim], axis=0)
                before = jnp.concatenate([brim, x], axis=0)
                rim = lax.broadcasted_iota(jnp.int32, (part // sub + 1, sub, lane), 1)
                x = jnp.where(rim >= drop, after, before).reshape(part + sub, lane)
                half, cols = self.block_of(base, c)
                spot = (half, d, pl.ds(pl.multiple_of(over + r, sub), part + sub), cols)
                self.tot[spot] = self.tot[spot] + x

        return [functools.partial(unit, d, r) for r in range(0, width, part) for d in range(2)]

    def left(self, kind, m):
        n, h = ROWS_OF_CHUNK, self.h
        rhs, lhs = (self.psi, self.a) if kind == "L1" else (self.chi, self.b)
        reg = self.flip
        self.flip = 1 - reg

        def push():
            for unit in range(2):
                pltpu.matmul_push_rhs(rhs[m % 2, unit], reg, unit)

        def feed(r, first):
            for unit in range(2):
                self.acc.feed(unit, (kind, m, r), lhs[unit, r : r + n], reg if first else None)

        order = [r + d for r in range(0, h, n) for d in (0, h)]
        return push, [functools.partial(feed, r, k == 0) for k, r in enumerate(order)]

    def right(self, kind, m):
        n, h = ROWS_OF_CHUNK, self.h
        rhs = self.b if kind == "R1" else self.a
        reg = self.flip
        self.flip = 1 - reg

        def push():
            for unit in range(2):
                pltpu.matmul_push_rhs(rhs[unit], reg, unit)

        def feed_forward(r, p, first):
            re, im = self.acc.pop(p, ("L1", m, r)), self.acc.pop(p, ("L1", m, h + r))
            re_l, re_r, im_l, im_r = re[:, :h], re[:, h:], im[:, :h], im[:, h:]
            plus = jnp.concatenate([re_l + re_r, im_l + im_r], axis=1).astype(jnp.bfloat16)
            less = jnp.concatenate([re_l - re_r, im_l - im_r], axis=1).astype(jnp.bfloat16)
            for unit, x in enumerate((plus, less)):
                self.acc.feed(unit, (kind, m, p * h + r), x, reg if first else None)

        def feed_backward(r, first):
            key = ("L2", m, r), ("L2", m, h + r)
            ere, oim = self.acc.pop(0, key[0]), self.acc.pop(1, key[1])
            ore, eim = self.acc.pop(1, key[0]), self.acc.pop(0, key[1])
            for k, (re, im) in enumerate(((ere + ore, eim + oim), (ere - ore, eim - oim))):
                for unit in range(2):
                    cols = slice(unit * h, (unit + 1) * h)
                    y = jnp.concatenate([re[:, cols], im[:, cols]], axis=1).astype(jnp.bfloat16)
                    self.acc.feed(
                        unit, (kind, m, k * h + r), y, reg if first and k == 0 else None
                    )

        if kind == "R1":
            spots = [(r, p) for r in range(0, h, n) for p in range(2)]
            feeds = [functools.partial(feed_forward, r, p, k == 0) for k, (r, p) in enumerate(spots)]
        else:
            feeds = [functools.partial(feed_backward, r, r == 0) for r in range(0, h, n)]
        return push, feeds

    def run(self, jobs):
        built = []
        for kind, m, beside in jobs:
            if kind is None:
                built.append((None, [], beside))
                continue
            push, feeds = (self.left if kind[0] == "L" else self.right)(kind, m)
            built.append((push, feeds, beside))
        for k, (push, feeds, beside) in enumerate(built):
            if push is not None and (k == 0 or built[k - 1][0] is None):
                push()
            for unit in interleave(beside, feeds):
                unit()
            if push is not None and k + 1 < len(built) and built[k + 1][0] is not None:
                built[k + 1][0]()


def forward_only(step, s, ahead, blank):
    psi, weigh = step.make_psi, lambda m: step.weigh(m, s)
    for unit in step.cut_patch(s) + psi(0):
        unit()
    step.run(
        [
            ("L1", 0, psi(1)),
            ("L1", 1, psi(2)),
            ("R1", 0, psi(3)),
            ("L1", 2, weigh(0)),
            ("R1", 1, step.cut_patch(ahead)),
            ("L1", 3, weigh(1) + blank[:16]),
            ("R1", 2, psi(0) + blank[16:]),
            ("R1", 3, weigh(2)),
            (None, 0, weigh(3)),
        ]
    )


def backward_only(step, s, behind):
    chi, gather, place = step.make_chi, step.gather, step.place(behind)
    half = len(place) // 2
    step.run(
        [
            (None, 0, chi(0)),
            ("L2", 0, chi(1) + place[:half]),
            ("L2", 1, chi(2) + place[half:]),
            ("R2", 0, []),
            ("L2", 2, chi(3) + gather(0)),
            ("R2", 1, []),
            ("L2", 3, gather(1)),
            ("R2", 2, []),
            ("R2", 3, gather(2)),
            (None, 0, gather(3) + step.place(s)),
        ]
    )


def both_ways(step, behind, back, ahead, beyond):
    psi, weigh = step.make_psi, lambda m: step.weigh(m, ahead)
    chi, gather = step.make_chi, step.gather
    cut, place = step.cut_patch(beyond), step.place(behind)
    psi1, psi2, psi3, psi0 = psi(1), psi(2), psi(3), psi(0)
    step.run(
        [
            ("L1", 0, interleave(chi(0), psi1[:3])),
            ("L2", 0, interleave(chi(1), psi1[3:])),
            ("L1", 1, place[:5]),
            ("R2", 0, place[5:]),
            ("L2", 1, psi2),
            ("R1", 0, gather(0)),
            ("R2", 1, chi(2)),
            ("L2", 2, interleave(chi(3), weigh(0))),
            ("L1", 2, psi3),
            ("R2", 2, gather(1)),
            ("L2", 3, cut),
            ("R1", 1, gather(2)),
            ("L1", 3, weigh(1)),
            ("R2", 3, psi0),
            ("R1", 2, []),
            ("R1", 3, interleave(gather(3), weigh(2))),
            (None, 0, weigh(3)),
        ]
    )


NAMES = ("count", "pos", "ext", "amp", "probe", "a", "b", "tot")
NAMES += ("patch", "psi", "far", "chi", "grad", "bright", "ratio")


def gradient_kernel(*operands):
    refs = dict(zip(NAMES, operands))
    tot = refs["tot"]

    def clear(half, d, r):
        part = 64
        tot[half, d, r : r + part] = jnp.zeros((part, tot.shape[3]), jnp.float32)

    blank = [
        functools.partial(clear, half, d, r)
        for half in range(2)
        for d in range(2)
        for r in range(0, tot.shape[2], 64)
    ]
    refs["grad"][...] = jnp.zeros_like(refs["grad"])
    count = refs["count"][0, 0]
    last = refs["amp"].shape[0] - 1

    def with_units(work, *where):
        def body(*acc):
            half = len(acc) // 2
            work(Step(refs, Chunks((acc[:half], acc[half:]))), *where)

        depth = 1024 // ROWS_OF_CHUNK
        shape = (ROWS_OF_CHUNK, refs["probe"].shape[-1])
        pl.run_scoped(body, *[pltpu.ACC(u)(shape, jnp.float32) for u in (0, 1) for _ in range(depth)])

    @pl.when(count > 0)
    def _():
        with_units(forward_only, 0, min(1, last), blank)

    @pl.when(count <= 0)
    def _():
        for unit in blank:
            unit()

    def one(s, carry):
        with_units(both_ways, jnp.maximum(s - 1, 0), s, s + 1, jnp.minimum(s + 2, last))
        return carry

    lax.fori_loop(0, count - 1, one, 0)

    @pl.when(count > 0)
    def _():
        with_units(backward_only, count - 1, jnp.maximum(count - 2, 0))


def gradient(counts, where, extended, amp, probe_modes, fwd, inv):
    modes, _, width, _ = probe_modes.shape
    vmem = pl.BlockSpec(memory_space=pltpu.VMEM)
    smem = pl.BlockSpec(memory_space=pltpu.SMEM)
    half = width // 2
    return pl.pallas_call(
        gradient_kernel,
        out_shape=jax.ShapeDtypeStruct(extended.shape, jnp.float32),
        in_specs=[smem, smem] + [vmem] * 5,
        out_specs=vmem,
        scratch_shapes=[
            pltpu.VMEM((2, width, width), jnp.float32),
            pltpu.VMEM((2, 2, width, width), jnp.bfloat16),
            pltpu.VMEM((modes, 2, width, width), jnp.float32),
            pltpu.VMEM((2, 2, width, width), jnp.bfloat16),
            pltpu.VMEM((2, width, width), jnp.float32),
            pltpu.VMEM((2, width, half), jnp.float32),
            pltpu.VMEM((2, width, half), jnp.float32),
        ],
        compiler_params=pltpu.CompilerParams(vmem_limit_bytes=40 * 1024 * 1024),
        name="gradient",
    )(counts, where, extended, amp, probe_modes, fwd, inv)


def exact(values, product):
    total = None
    for _ in range(3):
        piece = values.astype(jnp.bfloat16)
        values = values - piece.astype(jnp.float32)
        part = product(piece)
        total = part if total is None else total + part
    return total


def body(object_field, probe_modes, positions, counts, amplitude):
    width = probe_modes.shape[-1]
    fwd, inv = tables(width)
    where = positions[0, 0].T
    held = [
        pltpu.with_memory_space_constraint(x, pltpu.HBM)
        for x in (object_field, amplitude[0, 0], fwd, inv)
    ]
    extended, amp, fwd, inv = exchange("spread", *held)
    for sweep in range(ITERS):
        total = gradient(counts, where, extended, amp, probe_modes, fwd, inv)
        (extended,) = exchange("both" if sweep < ITERS - 1 else "reduce", total, extended)
    return extended


def solution(mesh):
    placed = (
        P(None, "row", "col"),
        P(),
        P("row", "col", None, None),
        P("row", "col"),
        P("row", "col", None, None, None),
    )
    return jax.shard_map(
        body, mesh=mesh, in_specs=placed, out_specs=P(None, "row", "col"), check_vma=False
    )
```
